16 devices in a mesh: my: 2 (over z), mx: 8 (over y, x, core).
Axes of the slice: x: 2, y: 2, z: 2, core: 2. Of those that a mesh axis runs over, the one named last changes fastest.
Arguments:
- x_in: bfloat16 [64, 5120], P(None, 'mx')
- seq_lens: int32 [64], P('mx')
- gain_attn: bfloat16 [5120], P('mx')
- gain_mlp: bfloat16 [5120], P('mx')
- w_q: bfloat16 [5120, 5120], P('mx', 'my')
- b_q: bfloat16 [5120], P('my')
- w_k: bfloat16 [5120, 1024], P('mx', 'my')
- b_k: bfloat16 [1024], P('my')
- w_v: bfloat16 [5120, 1024], P('mx', 'my')
- b_v: bfloat16 [1024], P('my')
- w_o: bfloat16 [5120, 5120], P('my', 'mx')
- w_gate: bfloat16 [5120, 27648], P('mx', 'my')
- w_up: bfloat16 [5120, 27648], P('mx', 'my')
- w_down: bfloat16 [27648, 5120], P('my', 'mx')
- k_cache: bfloat16 [64, 1024, 8, 128], P('mx', None, 'my')
- v_cache: bfloat16 [64, 1024, 8, 128], P('mx', None, 'my')
Outputs:
- output 1: bfloat16 [64, 5120], P(None, 'mx')
- output 2: bfloat16 [64, 1024, 8, 128], P('mx', None, 'my')
- output 3: bfloat16 [64, 1024, 8, 128], P('mx', None, 'my')
All inputs are finite; a program needn't handle non-finite values.
Results may differ from the reference program's by a relative error of at most 0.016982.
Values are sent between devices in bfloat16 or wider.
A program may use at most 1 GiB of HBM per device.

```python
import jax
import jax.numpy as jnp
from jax import lax

D = 5120
HEADS = 40
KV_HEADS = 8
HEAD = 128
FF = 27648
BATCH = 64
SEQ = 1024
NORM_EPS = 1e-6
ROPE_THETA = 1000000.0
GROUP = HEADS // KV_HEADS


def setup_inputs(seed: int = 0) -> dict:
    key_list = jax.random.split(jax.random.key(seed), 17)
    q_width = HEADS * HEAD
    kv_width = KV_HEADS * HEAD
    cache_shape = (BATCH, SEQ, KV_HEADS, HEAD)

    def normal(key_index, shape, scale, offset=0.0):
        samples = jax.random.normal(key_list[key_index], shape, jnp.float32)
        return (offset + scale * samples).astype(jnp.bfloat16)

    lens_draw = jax.random.randint(key_list[0], (BATCH,), 0, SEQ)
    full_row = jax.random.randint(key_list[1], (), 0, BATCH)
    seq_lens = jnp.where(jnp.arange(BATCH) == full_row, SEQ - 1, lens_draw).astype(jnp.int32)
    return {
        "x_in": normal(2, (BATCH, D), 1.0),
        "seq_lens": seq_lens,
        "gain_attn": normal(3, (D,), 0.3, 1.0),
        "gain_mlp": normal(4, (D,), 0.3, 1.0),
        "w_q": normal(5, (D, q_width), 2.0 * D ** -0.5),
        "b_q": normal(6, (q_width,), 1.0),
        "w_k": normal(7, (D, kv_width), D ** -0.5),
        "b_k": normal(8, (kv_width,), 1.0),
        "w_v": normal(9, (D, kv_width), D ** -0.5),
        "b_v": normal(10, (kv_width,), 1.0),
        "w_o": normal(11, (q_width, D), q_width ** -0.5),
        "w_gate": normal(12, (D, FF), D ** -0.5),
        "w_up": normal(13, (D, FF), D ** -0.5),
        "w_down": normal(14, (FF, D), FF ** -0.5),
        "k_cache": normal(15, cache_shape, 1.0),
        "v_cache": normal(16, cache_shape, 1.0),
    }


def rms_norm(rows_in, gain_vec):
    rows_f32 = rows_in.astype(jnp.float32)
    mean_sq = jnp.mean(rows_f32 * rows_f32, axis=-1, keepdims=True)
    return (rows_f32 * lax.rsqrt(mean_sq + NORM_EPS) * gain_vec.astype(jnp.float32)).astype(jnp.bfloat16)


def apply_rotary(vectors, positions):
    half_dim = HEAD // 2
    inv_freq = ROPE_THETA ** (-2.0 * jnp.arange(half_dim, dtype=jnp.float32) / HEAD)
    angles = positions.astype(jnp.float32)[:, None, None] * inv_freq
    cos_tab = jnp.cos(angles)
    sin_tab = jnp.sin(angles)
    lower_half = vectors[..., :half_dim]
    upper_half = vectors[..., half_dim:]
    return jnp.concatenate([lower_half * cos_tab - upper_half * sin_tab, upper_half * cos_tab + lower_half * sin_tab], axis=-1)


def attend_one(row_inputs):
    q_row, k_rows, v_rows, length = row_inputs
    q_grouped = q_row.reshape(KV_HEADS, GROUP, HEAD).astype(jnp.float32)
    scores = jnp.einsum("kgd,skd->kgs", q_grouped, k_rows.astype(jnp.float32)) * HEAD ** -0.5
    visible = (jnp.arange(SEQ) <= length)[None, None, :]
    scores = jnp.where(visible, scores, -jnp.inf)
    weights = jnp.exp(scores - jnp.max(scores, axis=-1, keepdims=True))
    weight_sum = jnp.sum(weights, axis=-1, keepdims=True)
    weighted = jnp.einsum("kgs,skd->kgd", weights.astype(jnp.bfloat16).astype(jnp.float32), v_rows.astype(jnp.float32))
    return (weighted / weight_sum).astype(jnp.bfloat16).reshape(HEADS * HEAD)


def reference(x_in, seq_lens, gain_attn, gain_mlp, w_q, b_q, w_k, b_k, w_v, b_v, w_o, w_gate, w_up, w_down, k_cache, v_cache):
    normed = rms_norm(x_in, gain_attn)
    q_vals = jnp.dot(normed, w_q, preferred_element_type=jnp.float32) + b_q.astype(jnp.float32)
    k_vals = jnp.dot(normed, w_k, preferred_element_type=jnp.float32) + b_k.astype(jnp.float32)
    v_vals = jnp.dot(normed, w_v, preferred_element_type=jnp.float32) + b_v.astype(jnp.float32)
    q_rot = apply_rotary(q_vals.reshape(BATCH, HEADS, HEAD), seq_lens).astype(jnp.bfloat16)
    k_rot = apply_rotary(k_vals.reshape(BATCH, KV_HEADS, HEAD), seq_lens).astype(jnp.bfloat16)
    v_new = v_vals.reshape(BATCH, KV_HEADS, HEAD).astype(jnp.bfloat16)
    at_slot = (jnp.arange(SEQ)[None, :] == seq_lens[:, None])[:, :, None, None]
    k_cache_out = jnp.where(at_slot, k_rot[:, None], k_cache)
    v_cache_out = jnp.where(at_slot, v_new[:, None], v_cache)
    attn_rows = lax.map(attend_one, (q_rot, k_cache_out, v_cache_out, seq_lens))
    x_mid = (x_in.astype(jnp.float32) + jnp.dot(attn_rows, w_o, preferred_element_type=jnp.float32)).astype(jnp.bfloat16)
    normed_mlp = rms_norm(x_mid, gain_mlp)
    gate_proj = jnp.dot(normed_mlp, w_gate, preferred_element_type=jnp.float32)
    up_proj = jnp.dot(normed_mlp, w_up, preferred_element_type=jnp.float32)
    hidden_act = (jax.nn.silu(gate_proj) * up_proj).astype(jnp.bfloat16)
    x_out = (x_mid.astype(jnp.float32) + jnp.dot(hidden_act, w_down, preferred_element_type=jnp.float32)).astype(jnp.bfloat16)
    return (x_out, k_cache_out, v_cache_out)
```

```python
import functools

import jax
import jax.numpy as jnp
from jax import lax
from jax.experimental import pallas as pl
from jax.experimental.pallas import tpu as pltpu
from jax.sharding import PartitionSpec as P

HEAD = 128
NORM_EPS = 1e-6
ROPE_THETA = 1000000.0
MESH = pl.DeviceIdType.MESH
F32 = jnp.float32
BF16 = jnp.bfloat16
VMEM = pltpu.VMEM
DMA = pltpu.SemaphoreType.DMA


def neighbours(mx):
    core = lax.rem(mx, 2)
    chip = mx // 2
    x_pos = lax.rem(chip, 2)
    y_pos = chip // 2
    others = (y_pos * 2 + (1 - x_pos), (1 - y_pos) * 2 + x_pos, (1 - y_pos) * 2 + (1 - x_pos))
    return core, chip, chip * 2 + (1 - core), others


def send(src, dst, send_sem, recv_sem, my, mx):
    copy = pltpu.make_async_remote_copy(src_ref=src, dst_ref=dst, send_sem=send_sem, recv_sem=recv_sem, device_id=(my, mx), device_id_type=MESH)
    copy.start()
    return copy


def drain(ref, sem):
    pltpu.make_async_copy(ref, ref, sem).wait()


def share_stat(square_sum, my, mx, stat_out, stat_in, send_sems, recv_sems):
    rows = square_sum.shape[0]
    turned = jnp.transpose(jnp.broadcast_to(square_sum, (rows, 128)))[0:8]
    stat_out[...] = turned
    copies = []
    for step in range(1, 8):
        peer = lax.rem(mx + step, 8)
        copies.append(send(stat_out, stat_in.at[mx], send_sems.at[step], recv_sems.at[step], my, peer))
    stat_in[mx] = turned
    for copy in copies:
        copy.wait()
    total = jnp.sum(stat_in[...], axis=0)
    return jnp.transpose(jnp.broadcast_to(total[0:1], (128, rows)))[:, 0:1]


def enter(my, mx, with_z):
    barrier = pltpu.get_barrier_semaphore()
    for step in range(1, 8):
        pl.semaphore_signal(barrier, inc=1, device_id=(my, lax.rem(mx + step, 8)), device_id_type=MESH)
    if with_z:
        pl.semaphore_signal(barrier, inc=1, device_id=(1 - my, mx), device_id_type=MESH)
    pl.semaphore_wait(barrier, 8 if with_z else 7)


def qkv_kernel(hidden, pieces, x_ref, gain_ref, wq_hbm, wk_hbm, wv_hbm, out_ref, wq_v, wk_v, wv_v, part, pair_in, chip_in, stat_out, stat_in,
               w_sems, stat_send, stat_recv, pair_send, pair_recv, chip_send, chip_recv):
    my = lax.axis_index("my")
    mx = lax.axis_index("mx")
    core, chip, partner, others = neighbours(mx)
    loads = [pltpu.make_async_copy(src, dst, w_sems.at[n]) for n, (src, dst) in enumerate(((wq_hbm, wq_v), (wk_hbm, wk_v), (wv_hbm, wv_v)))]
    for load in loads:
        load.start()
    enter(my, mx, False)
    x = x_ref[...].astype(F32)
    stat = share_stat(jnp.sum(x * x, axis=1, keepdims=True), my, mx, stat_out, stat_in, stat_send, stat_recv)
    normed = (x * lax.rsqrt(stat / hidden + NORM_EPS) * gain_ref[...].astype(F32)).astype(BF16)
    weights = (wq_v, wk_v, wv_v)
    copies = []
    waited = set()
    pair_copies = []
    for n, (which, first, width, out_first) in enumerate(pieces):
        if which not in waited:
            loads[which].wait()
            waited.add(which)
        cols = pl.ds(out_first, width)
        product = jnp.dot(normed, weights[which][:, first:first + width], preferred_element_type=F32)
        part[:, :, :, cols] = product.reshape(4, 2, 8, width).astype(BF16)
        pair_copies.append(send(part.at[:, 1 - core, :, cols], pair_in.at[:, :, cols], pair_send.at[n], pair_recv.at[n], my, partner))
    for n, (which, first, width, out_first) in enumerate(pieces):
        cols = pl.ds(out_first, width)
        pair_copies[n].wait_recv()
        pair_in[:, :, cols] = (part[:, core, :, cols].astype(F32) + pair_in[:, :, cols].astype(F32)).astype(BF16)
        for k, other in enumerate(others):
            copies.append(send(pair_in.at[other, :, cols], chip_in.at[k, :, cols], chip_send.at[n, k], chip_recv.at[n, k], my, other * 2 + core))
    for n, (which, first, width, out_first) in enumerate(pieces):
        cols = pl.ds(out_first, width)
        total = pair_in[chip, :, cols].astype(F32)
        for k in range(3):
            copies[n * 3 + k].wait_recv()
            total = total + chip_in[k, :, cols].astype(F32)
        out_ref[:, cols] = total
    for copy in pair_copies + copies:
        copy.wait_send()


def attend_kernel(lens_ref, proj_ref, bq_ref, bk_ref, bv_ref, cos_ref, sin_ref, k_hbm, v_hbm, ko_hbm, vo_hbm, attn_ref,
                  k_buf, v_buf, q_s, k_s, v_s, o_s, in_sems, out_sems):
    rows, slots, _ = k_buf.shape
    kv_heads = bk_ref.shape[0] // HEAD
    heads = bq_ref.shape[0] // HEAD
    group = heads // kv_heads
    q_cols = heads * HEAD
    kv_cols = kv_heads * HEAD
    for b in range(rows):
        pltpu.make_async_copy(k_hbm.at[b], k_buf.at[b], in_sems.at[0, b]).start()
        pltpu.make_async_copy(v_hbm.at[b], v_buf.at[b], in_sems.at[1, b]).start()
    cos = cos_ref[...]
    sin = sin_ref[...]
    q_s[...] = jnp.zeros_like(q_s)

    def biased(first, bias_ref, h):
        return proj_ref[:, first + h * HEAD:first + (h + 1) * HEAD] + bias_ref[h * HEAD:(h + 1) * HEAD].astype(F32)[None, :]

    def rotated(vals):
        return vals * cos + pltpu.roll(vals, HEAD // 2, 1) * sin

    for h in range(heads):
        q_s[:, h, :] = rotated(biased(0, bq_ref, h))
    for h in range(kv_heads):
        k_new = rotated(biased(q_cols, bk_ref, h))
        v_new = biased(q_cols + kv_cols, bv_ref, h)
        for r in range(16 // kv_heads):
            k_s[:, r * kv_heads + h, :] = k_new
            v_s[:, r * kv_heads + h, :] = v_new
    q_pad = q_s.shape[1]
    per_tile = 16 // kv_heads
    sub = lax.broadcasted_iota(jnp.int32, (16, HEAD), 0) // kv_heads
    col = lax.broadcasted_iota(jnp.int32, (q_pad, slots), 1)
    row = lax.broadcasted_iota(jnp.int32, (q_pad, slots), 0)
    row_head = sum((row >= group * n).astype(jnp.int32) for n in range(1, kv_heads))
    own_head = lax.rem(col, kv_heads) == row_head

    @pl.loop(0, rows)
    def _(b):
        position = lens_ref[b]
        base = pl.multiple_of(position // per_tile * 16, 16)
        at_slot = sub == lax.rem(position, per_tile)
        for buf, new, hbm, n in ((k_buf, k_s, k_hbm, 0), (v_buf, v_s, v_hbm, 1)):
            pltpu.make_async_copy(hbm.at[b], buf.at[b], in_sems.at[n, b]).wait()
            window = buf[b, pl.ds(base, 16), :].astype(F32)
            buf[b, pl.ds(base, 16), :] = jnp.where(at_slot, new[b], window).astype(BF16)
        scores = lax.dot_general(q_s[b].astype(BF16), k_buf[b], (((1,), (1,)), ((), ())), preferred_element_type=F32) * HEAD ** -0.5
        scores = jnp.where(own_head & (col < (position + 1) * kv_heads), scores, -jnp.inf)
        top = jnp.max(scores, axis=1, keepdims=True)
        top = jnp.where(top == -jnp.inf, 0.0, top)
        weights = jnp.exp(scores - top)
        weight_sum = jnp.sum(weights, axis=1, keepdims=True)
        weighted = jnp.dot(weights.astype(BF16), v_buf[b], preferred_element_type=F32)
        o_s[b] = weighted / weight_sum
        pltpu.make_async_copy(k_buf.at[b], ko_hbm.at[b], out_sems.at[0, b]).start()
        pltpu.make_async_copy(v_buf.at[b], vo_hbm.at[b], out_sems.at[1, b]).start()

    for h in range(heads):
        attn_ref[:, h * HEAD:(h + 1) * HEAD] = o_s[:, h, :].astype(BF16)
    for b in range(rows):
        pltpu.make_async_copy(k_buf.at[b], ko_hbm.at[b], out_sems.at[0, b]).wait()
        pltpu.make_async_copy(v_buf.at[b], vo_hbm.at[b], out_sems.at[1, b]).wait()


def mlp_kernel(hidden, chunks, per_load, attn_ref, x_ref, gain_ref, wo_hbm, wg_hbm, wu_hbm, wd_hbm, out_ref,
               attn_all, wo_v, wg_v, wu_v, wd_v, z_out, z_in, stat_out, stat_in, h_v, m_v, acc, mine, theirs, pair_in, chip_in, act,
               wo_sem, wg_sems, wu_sems, wd_sems, ag_send, ag_recv, z_send, z_recv, stat_send, stat_recv,
               pair_send, pair_recv, chip_send, chip_recv, act_send, act_recv, fwd_send, fwd_recv):
    my = lax.axis_index("my")
    mx = lax.axis_index("mx")
    core, chip, partner, others = neighbours(mx)
    half = act.shape[4]
    loads = chunks // per_load
    load_cols = per_load * 2 * half

    load_wo = pltpu.make_async_copy(wo_hbm, wo_v, wo_sem)
    load_wo.start()

    def load_gate(n):
        cols = pl.ds(pl.multiple_of(n * load_cols, 128), load_cols)
        return pltpu.make_async_copy(wg_hbm.at[:, cols], wg_v.at[n], wg_sems.at[n]), pltpu.make_async_copy(wu_hbm.at[:, cols], wu_v.at[n], wu_sems.at[n])

    def load_down(n):
        span = pl.ds(n * per_load, per_load)
        return pltpu.make_async_copy(wd_hbm.at[span], wd_v.at[span], wd_sems.at[n])

    @pl.loop(0, loads)
    def _(n):
        for load in load_gate(n):
            load.start()

    @pl.loop(0, loads)
    def _(n):
        load_down(n).start()

    enter(my, mx, True)

    copies = []
    for step in range(1, 8):
        peer = lax.rem(mx + step, 8)
        copies.append(send(attn_ref, attn_all.at[mx], ag_send.at[step], ag_recv.at[step], my, peer))
    attn_all[mx] = attn_ref[...]
    load_wo.wait()
    for copy in copies:
        copy.wait()
    rows = x_ref.shape[0]
    attn = attn_all[...].reshape(rows, attn_ref.shape[1])
    z_out[0] = jnp.dot(attn, wo_v[...], preferred_element_type=F32).astype(BF16)
    z_copy = send(z_out.at[0], z_in.at[0], z_send.at[0], z_recv.at[0], 1 - my, mx)
    z_copy.wait()
    mid = (x_ref[...].astype(F32) + (z_out[0].astype(F32) + z_in[0].astype(F32))).astype(BF16)
    m_v[...] = mid
    mid = mid.astype(F32)
    stat = share_stat(jnp.sum(mid * mid, axis=1, keepdims=True), my, mx, stat_out, stat_in, stat_send, stat_recv)
    h_v[...] = (mid * lax.rsqrt(stat / hidden + NORM_EPS) * gain_ref[...].astype(F32)).astype(BF16)
    acc[...] = jnp.zeros_like(acc)

    def products(k, part, dest):
        n = k // per_load
        cols = pl.ds(pl.multiple_of(lax.rem(k, per_load) * (2 * half) + part * half, 128), half)
        h = h_v[...]
        for which, weights in ((0, wg_v), (1, wu_v)):
            out = jnp.dot(h, weights[n, :, cols], preferred_element_type=F32)
            dest[k, :, which] = out.astype(BF16).reshape(4, 16, half)

    def multiply(k):
        @pl.when(lax.rem(k, per_load) == 0)
        def _():
            for load in load_gate(k // per_load):
                load.wait()

        products(k, 1 - core, theirs)
        send(theirs.at[k], pair_in.at[k], pair_send.at[k], pair_recv.at[k], my, partner)
        products(k, core, mine)

    def scatter(k):
        drain(pair_in.at[k], pair_recv.at[k])
        pair_in[k] = (mine[k].astype(F32) + pair_in[k].astype(F32)).astype(BF16)
        for n, other in enumerate(others):
            send(pair_in.at[k, other], chip_in.at[k, n], chip_send.at[k], chip_recv.at[k], my, other * 2 + core)

    def activate(k):
        drain(chip_in.at[k], chip_recv.at[k])
        total = pair_in[k, chip].astype(F32)
        for n in range(3):
            total = total + chip_in[k, n].astype(F32)
        gate = total[0]
        act[k, core, chip] = (gate * jax.nn.sigmoid(gate) * total[1]).astype(BF16)
        mine_act = act.at[k, core, chip]
        for other in others:
            send(mine_act, mine_act, act_send.at[k], act_recv.at[k], my, other * 2 + core)
        send(mine_act, mine_act, fwd_send.at[k], fwd_recv.at[k], my, partner)

    def forward(k):
        drain(act.at[k, core, pl.ds(0, 3)], act_recv.at[k])
        for other in others:
            block = act.at[k, core, other]
            send(block, block, fwd_send.at[k], fwd_recv.at[k], my, partner)

    def contract(k):
        @pl.when(lax.rem(k, per_load) == 0)
        def _():
            load_down(k // per_load).wait()

        drain(act.at[k, 1 - core], fwd_recv.at[k])
        total = acc[...]
        for part in range(2):
            total = total + jnp.dot(act[k, part].reshape(rows, half), wd_v[k, part], preferred_element_type=F32)
        acc[...] = total

    stages = ((contract, 10), (forward, 8), (activate, 5), (scatter, 2), (multiply, 0))

    @pl.loop(0, chunks + stages[0][1])
    def _(t):
        for stage, lag in stages:
            @pl.when(jnp.logical_and(t >= lag, t < chunks + lag))
            def _():
                stage(t - lag)

    z_out[1] = acc[...].astype(BF16)
    z_copy = send(z_out.at[1], z_in.at[1], z_send.at[1], z_recv.at[1], 1 - my, mx)
    z_copy.wait()
    out_ref[...] = (m_v[...].astype(F32) + (z_out[1].astype(F32) + z_in[1].astype(F32))).astype(BF16)

    @pl.loop(0, chunks)
    def _(k):
        drain(theirs.at[k], pair_send.at[k])
        drain(chip_in.at[k], chip_send.at[k])
        drain(act.at[k, core, pl.ds(0, 3)], act_send.at[k])
        drain(act.at[k, core], fwd_send.at[k])


def solution(mesh):
    mx_size = mesh.shape["mx"]
    act_spec = P(None, "mx")
    cache_spec = P("mx", None, "my", None)
    in_specs = (act_spec, P("mx"), P("mx"), P("mx"), P("mx", "my"), P("my"), P("mx", "my"), P("my"), P("mx", "my"), P("my"), P("my", "mx"), P("mx", "my"), P("mx", "my"), P("my", "mx"), cache_spec, cache_spec)
    out_specs = (act_spec, cache_spec, cache_spec)
    vmem = pl.BlockSpec(memory_space=pltpu.VMEM)
    smem = pl.BlockSpec(memory_space=pltpu.SMEM)
    anywhere = pl.BlockSpec(memory_space=pl.ANY)

    def local_layer(x_in, seq_lens, gain_attn, gain_mlp, w_q, b_q, w_k, b_k, w_v, b_v, w_o, w_gate, w_up, w_down, k_cache, v_cache):
        rows, cols = x_in.shape
        hidden = cols * mx_size
        q_cols = w_q.shape[1]
        kv_cols = w_k.shape[1]
        heads = q_cols // HEAD
        kv_heads = kv_cols // HEAD
        local_rows = rows // mx_size
        qkv_cols = q_cols + 2 * kv_cols
        pieces = ((0, 0, q_cols // 2, 0), (0, q_cols // 2, q_cols // 2, q_cols // 2), (1, 0, kv_cols, q_cols), (2, 0, kv_cols, q_cols + kv_cols))

        inv_freq = ROPE_THETA ** (-2.0 * jnp.arange(HEAD // 2, dtype=F32) / HEAD)
        angles = seq_lens.astype(F32)[:, None] * inv_freq
        cos_half = jnp.cos(angles)
        sin_half = jnp.sin(angles)
        cos_tab = jnp.concatenate([cos_half, cos_half], axis=1)
        sin_tab = jnp.concatenate([-sin_half, sin_half], axis=1)

        projected = pl.pallas_call(
            functools.partial(qkv_kernel, hidden, pieces),
            name="qkv",
            out_shape=jax.ShapeDtypeStruct((local_rows, qkv_cols), F32),
            in_specs=[vmem, vmem, anywhere, anywhere, anywhere],
            out_specs=vmem,
            scratch_shapes=[
                VMEM(w_q.shape, BF16), VMEM(w_k.shape, BF16), VMEM(w_v.shape, BF16),
                VMEM((4, 2, local_rows, qkv_cols), BF16), VMEM((4, local_rows, qkv_cols), BF16), VMEM((3, local_rows, qkv_cols), BF16),
                VMEM((8, rows), F32), VMEM((8, 8, rows), F32),
                DMA((3,)), DMA((8,)), DMA((8,)), DMA((4,)), DMA((4,)), DMA((4, 3)), DMA((4, 3)),
            ],
            compiler_params=pltpu.CompilerParams(collective_id=0, has_side_effects=True, vmem_limit_bytes=16 * 2 ** 20),
        )(x_in, gain_attn.reshape(1, cols), w_q, w_k, w_v)

        slots = k_cache.shape[1] * kv_heads
        flat = (local_rows, slots, HEAD)
        padded = (heads + 7) // 8 * 8
        k_flat, v_flat, attn = pl.pallas_call(
            attend_kernel,
            name="attend",
            out_shape=(jax.ShapeDtypeStruct(flat, BF16), jax.ShapeDtypeStruct(flat, BF16), jax.ShapeDtypeStruct((local_rows, q_cols), BF16)),
            in_specs=[smem, vmem, vmem, vmem, vmem, vmem, vmem, anywhere, anywhere],
            out_specs=(anywhere, anywhere, vmem),
            scratch_shapes=[
                VMEM(flat, BF16), VMEM(flat, BF16),
                VMEM((local_rows, padded, HEAD), F32), VMEM((local_rows, 16, HEAD), F32), VMEM((local_rows, 16, HEAD), F32), VMEM((local_rows, padded, HEAD), F32),
                DMA((2, local_rows)), DMA((2, local_rows)),
            ],
            compiler_params=pltpu.CompilerParams(vmem_limit_bytes=40 * 2 ** 20),
        )(seq_lens, projected, b_q, b_k, b_v, cos_tab, sin_tab, k_cache.reshape(flat), v_cache.reshape(flat))

        ff_cols = w_gate.shape[1]
        half = 256
        chunks = ff_cols // (2 * half)
        per_load = 3
        loads = chunks // per_load
        x_out = pl.pallas_call(
            functools.partial(mlp_kernel, hidden, chunks, per_load),
            name="mlp",
            out_shape=jax.ShapeDtypeStruct((rows, cols), BF16),
            in_specs=[vmem, vmem, vmem, anywhere, anywhere, anywhere, anywhere],
            out_specs=vmem,
            scratch_shapes=[
                VMEM((8, local_rows, q_cols), BF16), VMEM(w_o.shape, BF16),
                VMEM((loads, cols, per_load * 2 * half), BF16), VMEM((loads, cols, per_load * 2 * half), BF16), VMEM((chunks, 2, half, cols), BF16),
                VMEM((2, rows, cols), BF16), VMEM((2, rows, cols), BF16), VMEM((8, rows), F32), VMEM((8, 8, rows), F32),
                VMEM((rows, cols), BF16), VMEM((rows, cols), BF16), VMEM((rows, cols), F32),
                VMEM((chunks, 4, 2, 16, half), BF16), VMEM((chunks, 4, 2, 16, half), BF16), VMEM((chunks, 4, 2, 16, half), BF16),
                VMEM((chunks, 3, 2, 16, half), BF16), VMEM((chunks, 2, 4, 16, half), BF16),
                DMA, DMA((loads,)), DMA((loads,)), DMA((loads,)), DMA((8,)), DMA((8,)), DMA((2,)), DMA((2,)), DMA((8,)), DMA((8,)),
                DMA((chunks,)), DMA((chunks,)), DMA((chunks,)), DMA((chunks,)), DMA((chunks,)), DMA((chunks,)), DMA((chunks,)), DMA((chunks,)),
            ],
            compiler_params=pltpu.CompilerParams(collective_id=1, has_side_effects=True, vmem_limit_bytes=67043328),
        )(attn, x_in, gain_mlp.reshape(1, cols), w_o, w_gate, w_up, w_down.reshape(chunks, 2, half, cols))
        return x_out, k_flat.reshape(k_cache.shape), v_flat.reshape(v_cache.shape)

    return jax.shard_map(local_layer, mesh=mesh, in_specs=in_specs, out_specs=out_specs, check_vma=False)
```

```python
import functools

import jax
import jax.numpy as jnp
from jax import lax
from jax.experimental import pallas as pl
from jax.experimental.pallas import tpu as pltpu
from jax.sharding import PartitionSpec as P

HEAD = 128
NORM_EPS = 1e-6
ROPE_THETA = 1000000.0
MESH = pl.DeviceIdType.MESH
F32 = jnp.float32
BF16 = jnp.bfloat16
VMEM = pltpu.VMEM
DMA = pltpu.SemaphoreType.DMA


def neighbours(mx):
    core = lax.rem(mx, 2)
    chip = mx // 2
    x_pos = lax.rem(chip, 2)
    y_pos = chip // 2
    others = (y_pos * 2 + (1 - x_pos), (1 - y_pos) * 2 + x_pos, (1 - y_pos) * 2 + (1 - x_pos))
    return core, chip, chip * 2 + (1 - core), others


def hbm(array):
    return pltpu.with_memory_space_constraint(array, pltpu.HBM)


def send(src, dst, send_sem, recv_sem, my, mx):
    copy = pltpu.make_async_remote_copy(src_ref=src, dst_ref=dst, send_sem=send_sem, recv_sem=recv_sem, device_id=(my, mx), device_id_type=MESH)
    copy.start()
    return copy


def drain(ref, sem):
    pltpu.make_async_copy(ref, ref, sem).wait()


def share_stat(square_sum, my, mx, stat_out, stat_in, send_sems, recv_sems):
    rows = square_sum.shape[0]
    turned = jnp.transpose(jnp.broadcast_to(square_sum, (rows, 128)))[0:8]
    stat_out[...] = turned
    copies = []
    for step in range(1, 8):
        peer = lax.rem(mx + step, 8)
        copies.append(send(stat_out, stat_in.at[mx], send_sems.at[step], recv_sems.at[step], my, peer))
    stat_in[mx] = turned
    for copy in copies:
        copy.wait()
    total = jnp.sum(stat_in[...], axis=0)
    return jnp.transpose(jnp.broadcast_to(total[0:1], (128, rows)))[:, 0:1]


def enter(my, mx, with_z):
    barrier = pltpu.get_barrier_semaphore()
    for step in range(1, 8):
        pl.semaphore_signal(barrier, inc=1, device_id=(my, lax.rem(mx + step, 8)), device_id_type=MESH)
    if with_z:
        pl.semaphore_signal(barrier, inc=1, device_id=(1 - my, mx), device_id_type=MESH)
    pl.semaphore_wait(barrier, 8 if with_z else 7)


def qkv_kernel(hidden, pieces, freq_ref, lens_hbm, x_hbm, gain_hbm, wq_hbm, wk_hbm, wv_hbm, out_ref, cos_ref, sin_ref,
               lens_s, x_v, gain_v, wq_v, wk_v, wv_v, part, pair_in, chip_in, stat_out, stat_in,
               w_sems, stat_send, stat_recv, pair_send, pair_recv, chip_send, chip_recv):
    my = lax.axis_index("my")
    mx = lax.axis_index("mx")
    core, chip, partner, others = neighbours(mx)
    loads = [pltpu.make_async_copy(src, dst, w_sems.at[n]) for n, (src, dst) in enumerate((
        (wq_hbm, wq_v), (wk_hbm, wk_v), (wv_hbm, wv_v), (x_hbm, x_v), (gain_hbm, gain_v), (lens_hbm, lens_s)))]
    for n in (3, 4, 5, 0, 1, 2):
        loads[n].start()
    enter(my, mx, False)
    loads[3].wait()
    x = x_v[...].astype(F32)
    square_sum = jnp.sum(x * x, axis=1, keepdims=True)
    loads[4].wait()
    loads[5].wait()
    rows = lens_s.shape[0]
    sub = lax.broadcasted_iota(jnp.int32, (rows, HEAD // 2), 0)
    position = jnp.zeros((rows, HEAD // 2), F32)
    for b in range(rows):
        position = jnp.where(sub == b, lens_s[b].astype(F32), position)
    angles = position * freq_ref[...][None, :]
    cos_half = jnp.cos(angles)
    sin_half = jnp.sin(angles)
    cos_ref[...] = jnp.concatenate([cos_half, cos_half], axis=1)
    sin_ref[...] = jnp.concatenate([-sin_half, sin_half], axis=1)
    stat = share_stat(square_sum, my, mx, stat_out, stat_in, stat_send, stat_recv)
    normed = (x * lax.rsqrt(stat / hidden + NORM_EPS) * gain_v[...].astype(F32)[None, :]).astype(BF16)
    weights = (wq_v, wk_v, wv_v)
    copies = []
    waited = set()
    pair_copies = []
    for n, (which, first, width, out_first) in enumerate(pieces):
        if which not in waited:
            loads[which].wait()
            waited.add(which)
        cols = pl.ds(out_first, width)
        product = jnp.dot(normed, weights[which][:, first:first + width], preferred_element_type=F32)
        part[:, :, :, cols] = product.reshape(4, 2, 8, width).astype(BF16)
        pair_copies.append(send(part.at[:, 1 - core, :, cols], pair_in.at[:, :, cols], pair_send.at[n], pair_recv.at[n], my, partner))
    for n, (which, first, width, out_first) in enumerate(pieces):
        cols = pl.ds(out_first, width)
        pair_copies[n].wait_recv()
        pair_in[:, :, cols] = (part[:, core, :, cols].astype(F32) + pair_in[:, :, cols].astype(F32)).astype(BF16)
        for k, other in enumerate(others):
            copies.append(send(pair_in.at[other, :, cols], chip_in.at[k, :, cols], chip_send.at[n, k], chip_recv.at[n, k], my, other * 2 + core))
    for n, (which, first, width, out_first) in enumerate(pieces):
        cols = pl.ds(out_first, width)
        total = pair_in[chip, :, cols].astype(F32)
        for k in range(3):
            copies[n * 3 + k].wait_recv()
            total = total + chip_in[k, :, cols].astype(F32)
        out_ref[:, cols] = total
    for copy in pair_copies + copies:
        copy.wait_send()


def attend_kernel(proj_ref, cos_ref, sin_ref, k_ref, v_ref, lens_hbm, bq_hbm, bk_hbm, bv_hbm, ko_hbm, vo_hbm, attn_ref,
                  lens_s, bq_v, bk_v, bv_v, q_s, k_s, v_s, o_s, k_win, v_win, small_sems, out_sems, win_sems):
    rows, slots, _ = k_ref.shape
    kv_heads = bk_v.shape[0] // HEAD
    heads = bq_v.shape[0] // HEAD
    group = heads // kv_heads
    q_cols = heads * HEAD
    kv_cols = kv_heads * HEAD
    smalls = [pltpu.make_async_copy(src, dst, small_sems.at[n]) for n, (src, dst) in enumerate(((bq_hbm, bq_v), (bk_hbm, bk_v), (bv_hbm, bv_v), (lens_hbm, lens_s)))]
    for small in smalls:
        small.start()
    outs = []
    for b in range(rows):
        outs.append((pltpu.make_async_copy(k_ref.at[b], ko_hbm.at[b], out_sems.at[0, b]), pltpu.make_async_copy(v_ref.at[b], vo_hbm.at[b], out_sems.at[1, b])))
        for out in outs[b]:
            out.start()
    cos = cos_ref[...]
    sin = sin_ref[...]
    q_s[...] = jnp.zeros_like(q_s)
    for small in smalls:
        small.wait()

    def biased(first, bias_ref, h):
        return proj_ref[:, first + h * HEAD:first + (h + 1) * HEAD] + bias_ref[h * HEAD:(h + 1) * HEAD].astype(F32)[None, :]

    def rotated(vals):
        return vals * cos + pltpu.roll(vals, HEAD // 2, 1) * sin

    for h in range(heads):
        q_s[:, h, :] = rotated(biased(0, bq_v, h))
    for h in range(kv_heads):
        k_new = rotated(biased(q_cols, bk_v, h))
        v_new = biased(q_cols + kv_cols, bv_v, h)
        for r in range(16 // kv_heads):
            k_s[:, r * kv_heads + h, :] = k_new
            v_s[:, r * kv_heads + h, :] = v_new
    q_pad = q_s.shape[1]
    per_tile = 16 // kv_heads
    sub = lax.broadcasted_iota(jnp.int32, (16, HEAD), 0) // kv_heads
    row = lax.broadcasted_iota(jnp.int32, (q_pad, 1), 0)
    row_head = sum((row >= group * n).astype(jnp.int32) for n in range(1, kv_heads))
    col = lax.broadcasted_iota(jnp.int32, (q_pad, slots), 1)
    offset = jnp.where(lax.rem(col, kv_heads) == row_head, col // kv_heads, slots)
    new_col = lax.broadcasted_iota(jnp.int32, (q_pad, 16), 1)

    def window(b, position):
        base = pl.multiple_of(position // per_tile * 16, 16)
        at_slot = sub == lax.rem(position, per_tile)
        for src, new, win in ((k_ref, k_s, k_win), (v_ref, v_s, v_win)):
            win[b] = jnp.where(at_slot, new[b], src[b, pl.ds(base, 16), :].astype(F32)).astype(BF16)

    def one_row(b):
        position = lens_s[b]
        window(b, position)
        query = q_s[b].astype(BF16)
        scores = lax.dot_general(query, k_ref[b], (((1,), (1,)), ((), ())), preferred_element_type=F32) * HEAD ** -0.5
        scores = jnp.where(offset < position, scores, -jnp.inf)
        new_scores = lax.dot_general(query, k_s[b].astype(BF16), (((1,), (1,)), ((), ())), preferred_element_type=F32) * HEAD ** -0.5
        new_scores = jnp.where(new_col == row_head, new_scores, -jnp.inf)
        top = jnp.maximum(jnp.max(scores, axis=1, keepdims=True), jnp.max(new_scores, axis=1, keepdims=True))
        weights = jnp.exp(scores - top)
        new_weights = jnp.exp(new_scores - top)
        weight_sum = jnp.sum(weights, axis=1, keepdims=True) + jnp.sum(new_weights, axis=1, keepdims=True)
        weighted = jnp.dot(weights.astype(BF16), v_ref[b], preferred_element_type=F32)
        weighted = weighted + jnp.dot(new_weights.astype(BF16), v_s[b].astype(BF16), preferred_element_type=F32)
        o_s[b] = weighted / weight_sum

    def fix(b):
        base = pl.multiple_of(lens_s[b] // per_tile * 16, 16)
        return [pltpu.make_async_copy(win.at[b], hbm_out.at[b, pl.ds(base, 16), :], win_sems.at[n, b]) for n, (win, hbm_out) in enumerate(((k_win, ko_hbm), (v_win, vo_hbm)))]

    @pl.loop(0, rows, unroll=8)
    def _(b):
        one_row(b)

    for b in range(rows):
        for out, win in zip(outs[b], fix(b)):
            out.wait()
            win.start()
    for h in range(heads):
        attn_ref[:, h * HEAD:(h + 1) * HEAD] = o_s[:, h, :].astype(BF16)
    for b in range(rows):
        for win in fix(b):
            win.wait()


def mlp_kernel(hidden, chunks, per_load, lags, attn_ref, x_hbm, gain_hbm, wo_hbm, wg_hbm, wu_hbm, wd_hbm, out_ref,
               x_v, gain_v, attn_all, wo_v, wg_v, wu_v, wd_v, z_out, z_in, stat_out, stat_in, h_v, m_v, acc, mine, theirs, pair_in, hop_in, fin_in, act,
               in_sems, wg_sems, wu_sems, wd_sems, ag_send, ag_recv, z_send, z_recv, stat_send, stat_recv,
               pair_send, pair_recv, hop_send, hop_recv, fin_send, fin_recv, near_send, near_recv, far_send, far_recv, fwd_send, fwd_recv):
    my = lax.axis_index("my")
    mx = lax.axis_index("mx")
    core, chip, partner, others = neighbours(mx)
    x_pos = lax.rem(chip, 2)
    y_pos = chip // 2
    x_peer = others[0] * 2 + core
    y_peer = others[1] * 2 + core
    half = 2 * act.shape[6]
    loads = chunks // per_load
    load_cols = per_load * 2 * half
    ring = wd_v.shape[0]

    firsts = [pltpu.make_async_copy(src, dst, in_sems.at[n]) for n, (src, dst) in enumerate(((wo_hbm, wo_v), (x_hbm, x_v), (gain_hbm, gain_v)))]
    for first in firsts:
        first.start()

    def load_gate(n):
        cols = pl.ds(pl.multiple_of(n * load_cols, 128), load_cols)
        return pltpu.make_async_copy(wg_hbm.at[:, cols], wg_v.at[n], wg_sems.at[n]), pltpu.make_async_copy(wu_hbm.at[:, cols], wu_v.at[n], wu_sems.at[n])

    def load_down(n):
        slot = lax.rem(n, ring)
        return pltpu.make_async_copy(wd_hbm.at[n], wd_v.at[slot], wd_sems.at[slot])

    @pl.loop(0, loads)
    def _(n):
        for load in load_gate(n):
            load.start()

    for n in range(ring):
        load_down(n).start()

    enter(my, mx, True)

    copies = []
    for step in range(1, 8):
        peer = lax.rem(mx + step, 8)
        copies.append(send(attn_ref, attn_all.at[mx], ag_send.at[step], ag_recv.at[step], my, peer))
    attn_all[mx] = attn_ref[...]
    for first in firsts:
        first.wait()
    for copy in copies:
        copy.wait()
    rows = x_v.shape[0]
    attn = attn_all[...].reshape(rows, attn_ref.shape[1])
    z_out[0] = jnp.dot(attn, wo_v[...], preferred_element_type=F32).astype(BF16)
    z_copy = send(z_out.at[0], z_in.at[0], z_send.at[0], z_recv.at[0], 1 - my, mx)
    z_copy.wait()
    mid = (x_v[...].astype(F32) + (z_out[0].astype(F32) + z_in[0].astype(F32))).astype(BF16)
    m_v[...] = mid
    mid = mid.astype(F32)
    stat = share_stat(jnp.sum(mid * mid, axis=1, keepdims=True), my, mx, stat_out, stat_in, stat_send, stat_recv)
    h_v[...] = (mid * lax.rsqrt(stat / hidden + NORM_EPS) * gain_v[...].astype(F32)[None, :]).astype(BF16)
    acc[...] = jnp.zeros_like(acc)

    def products(k, part, dest):
        n = k // per_load
        cols = pl.ds(pl.multiple_of(lax.rem(k, per_load) * (2 * half) + part * half, 128), half)
        h = h_v[...]
        for which, weights in ((0, wg_v), (1, wu_v)):
            out = jnp.dot(h, weights[n, :, cols], preferred_element_type=F32).astype(BF16)
            for way in range(2):
                dest[k, way, :, :, which] = out[:, way * half // 2:(way + 1) * half // 2].reshape(2, 2, 16, half // 2)

    def multiply(k):
        @pl.when(lax.rem(k, per_load) == 0)
        def _():
            for load in load_gate(k // per_load):
                load.wait()

        products(k, 1 - core, theirs)
        send(theirs.at[k], pair_in.at[k], pair_send.at[k], pair_recv.at[k], my, partner)
        products(k, core, mine)

    def scatter(k):
        drain(pair_in.at[k], pair_recv.at[k])
        pair_in[k] = (mine[k].astype(F32) + pair_in[k].astype(F32)).astype(BF16)
        send(pair_in.at[k, 0, :, 1 - x_pos], hop_in.at[k, 0], hop_send.at[k], hop_recv.at[k], my, x_peer)
        send(pair_in.at[k, 1, 1 - y_pos], hop_in.at[k, 1], hop_send.at[k], hop_recv.at[k], my, y_peer)

    def combine(k):
        drain(hop_in.at[k], hop_recv.at[k])
        hop_in[k, 0] = (pair_in[k, 0, :, x_pos].astype(F32) + hop_in[k, 0].astype(F32)).astype(BF16)
        hop_in[k, 1] = (pair_in[k, 1, y_pos].astype(F32) + hop_in[k, 1].astype(F32)).astype(BF16)
        send(hop_in.at[k, 0, 1 - y_pos], fin_in.at[k, 0], fin_send.at[k], fin_recv.at[k], my, y_peer)
        send(hop_in.at[k, 1, 1 - x_pos], fin_in.at[k, 1], fin_send.at[k], fin_recv.at[k], my, x_peer)

    def activate(k):
        drain(fin_in.at[k], fin_recv.at[k])
        for way, own in ((0, y_pos), (1, x_pos)):
            total = hop_in[k, way, own].astype(F32) + fin_in[k, way].astype(F32)
            gate = total[0]
            act[k, core, way, y_pos, x_pos] = (gate * jax.nn.sigmoid(gate) * total[1]).astype(BF16)
        for way, peer in ((0, y_peer), (1, x_peer)):
            block = act.at[k, core, way, y_pos, x_pos]
            send(block, block, near_send.at[k], near_recv.at[k], my, peer)
        both = act.at[k, core, :, y_pos, x_pos]
        send(both, both, fwd_send.at[k], fwd_recv.at[k], my, partner)

    def gather(k):
        drain(act.at[k, core, 0, 0], near_recv.at[k])
        for block, peer in ((act.at[k, core, 0, :, x_pos], x_peer), (act.at[k, core, 1, y_pos], y_peer)):
            send(block, block, far_send.at[k], far_recv.at[k], my, peer)
        for block in (act.at[k, core, 0, 1 - y_pos, x_pos], act.at[k, core, 1, y_pos, 1 - x_pos]):
            send(block, block, fwd_send.at[k], fwd_recv.at[k], my, partner)

    def forward(k):
        drain(act.at[k, core, 0], far_recv.at[k])
        for block in (act.at[k, core, 0, :, 1 - x_pos], act.at[k, core, 1, 1 - y_pos]):
            send(block, block, fwd_send.at[k], fwd_recv.at[k], my, partner)

    def contract(k):
        n = k // per_load
        step = lax.rem(k, per_load)

        @pl.when(step == 0)
        def _():
            load_down(n).wait()

        drain(act.at[k, 1 - core], fwd_recv.at[k])
        total = acc[...]
        for part in range(2):
            lhs = jnp.concatenate([act[k, part, way].reshape(rows, half // 2) for way in range(2)], axis=1)
            total = total + jnp.dot(lhs, wd_v[lax.rem(n, ring), step, part], preferred_element_type=F32)
        acc[...] = total

        @pl.when(jnp.logical_and(step == per_load - 1, n + ring < loads))
        def _():
            load_down(n + ring).start()

    stages = tuple(zip((contract, forward, gather, activate, combine, scatter, multiply), lags))

    @pl.loop(0, chunks + lags[0])
    def _(t):
        for stage, lag in stages:
            @pl.when(jnp.logical_and(t >= lag, t < chunks + lag))
            def _():
                stage(t - lag)

    z_out[1] = acc[...].astype(BF16)
    z_copy = send(z_out.at[1], z_in.at[1], z_send.at[1], z_recv.at[1], 1 - my, mx)
    z_copy.wait()
    out_ref[...] = (m_v[...].astype(F32) + (z_out[1].astype(F32) + z_in[1].astype(F32))).astype(BF16)

    @pl.loop(0, chunks)
    def _(k):
        drain(theirs.at[k], pair_send.at[k])
        drain(hop_in.at[k], hop_send.at[k])
        drain(fin_in.at[k], fin_send.at[k])
        drain(act.at[k, core, 0, 0], near_send.at[k])
        drain(act.at[k, core, 0], far_send.at[k])
        drain(act.at[k, core], fwd_send.at[k])


def solution(mesh):
    mx_size = mesh.shape["mx"]
    act_spec = P(None, "mx")
    cache_spec = P("mx", None, "my", None)
    in_specs = (act_spec, P("mx"), P("mx"), P("mx"), P("mx", "my"), P("my"), P("mx", "my"), P("my"), P("mx", "my"), P("my"), P("my", "mx"), P("mx", "my"), P("mx", "my"), P("my", "mx"), cache_spec, cache_spec)
    out_specs = (act_spec, cache_spec, cache_spec)
    vmem = pl.BlockSpec(memory_space=pltpu.VMEM)
    anywhere = pl.BlockSpec(memory_space=pl.ANY)

    def local_layer(x_in, seq_lens, gain_attn, gain_mlp, w_q, b_q, w_k, b_k, w_v, b_v, w_o, w_gate, w_up, w_down, k_cache, v_cache):
        rows, cols = x_in.shape
        hidden = cols * mx_size
        q_cols = w_q.shape[1]
        kv_cols = w_k.shape[1]
        heads = q_cols // HEAD
        kv_heads = kv_cols // HEAD
        local_rows = rows // mx_size
        qkv_cols = q_cols + 2 * kv_cols
        pieces = ((0, 0, q_cols // 2, 0), (0, q_cols // 2, q_cols // 2, q_cols // 2), (1, 0, kv_cols, q_cols), (2, 0, kv_cols, q_cols + kv_cols))
        inv_freq = ROPE_THETA ** (-2.0 * jnp.arange(HEAD // 2, dtype=F32) / HEAD)
        table = jax.ShapeDtypeStruct((local_rows, HEAD), F32)

        projected, cos_tab, sin_tab = pl.pallas_call(
            functools.partial(qkv_kernel, hidden, pieces),
            name="qkv",
            out_shape=(jax.ShapeDtypeStruct((local_rows, qkv_cols), F32), table, table),
            in_specs=[vmem] + [anywhere] * 6,
            out_specs=(vmem, vmem, vmem),
            scratch_shapes=[
                pltpu.SMEM((local_rows,), jnp.int32), VMEM((rows, cols), BF16), VMEM((cols,), BF16),
                VMEM(w_q.shape, BF16), VMEM(w_k.shape, BF16), VMEM(w_v.shape, BF16),
                VMEM((4, 2, local_rows, qkv_cols), BF16), VMEM((4, local_rows, qkv_cols), BF16), VMEM((3, local_rows, qkv_cols), BF16),
                VMEM((8, rows), F32), VMEM((8, 8, rows), F32),
                DMA((6,)), DMA((8,)), DMA((8,)), DMA((4,)), DMA((4,)), DMA((4, 3)), DMA((4, 3)),
            ],
            compiler_params=pltpu.CompilerParams(collective_id=0, has_side_effects=True, vmem_limit_bytes=16 * 2 ** 20),
            cost_estimate=pl.CostEstimate(flops=40_000_000_000, bytes_accessed=4_600_000, transcendentals=0),
        )(inv_freq, hbm(seq_lens), hbm(x_in), hbm(gain_attn), hbm(w_q), hbm(w_k), hbm(w_v))

        slots = k_cache.shape[1] * kv_heads
        flat = (local_rows, slots, HEAD)
        padded = (heads + 7) // 8 * 8
        k_flat, v_flat, attn = pl.pallas_call(
            attend_kernel,
            name="attend",
            out_shape=(jax.ShapeDtypeStruct(flat, BF16), jax.ShapeDtypeStruct(flat, BF16), jax.ShapeDtypeStruct((local_rows, q_cols), BF16)),
            in_specs=[vmem] * 5 + [anywhere] * 4,
            out_specs=(anywhere, anywhere, vmem),
            scratch_shapes=[
                pltpu.SMEM((local_rows,), jnp.int32), VMEM(b_q.shape, BF16), VMEM(b_k.shape, BF16), VMEM(b_v.shape, BF16),
                VMEM((local_rows, padded, HEAD), F32), VMEM((local_rows, 16, HEAD), F32), VMEM((local_rows, 16, HEAD), F32), VMEM((local_rows, padded, HEAD), F32),
                VMEM((local_rows, 16, HEAD), BF16), VMEM((local_rows, 16, HEAD), BF16),
                DMA((4,)), DMA((2, local_rows)), DMA((2, local_rows)),
            ],
            compiler_params=pltpu.CompilerParams(vmem_limit_bytes=26 * 2 ** 20),
            cost_estimate=pl.CostEstimate(flops=20_000_000_000, bytes_accessed=17_000_000, transcendentals=0),
        )(projected, cos_tab, sin_tab, pltpu.with_memory_space_constraint(k_cache.reshape(flat), VMEM), pltpu.with_memory_space_constraint(v_cache.reshape(flat), VMEM),
          hbm(seq_lens), hbm(b_q), hbm(b_k), hbm(b_v))

        ff_cols = w_gate.shape[1]
        half = 256
        chunks = ff_cols // (2 * half)
        per_load = 3
        ring = 3
        loads = chunks // per_load
        lags = (28, 25, 20, 14, 8, 2, 0)
        x_out = pl.pallas_call(
            functools.partial(mlp_kernel, hidden, chunks, per_load, lags),
            name="mlp",
            out_shape=jax.ShapeDtypeStruct((rows, cols), BF16),
            in_specs=[vmem] + [anywhere] * 6,
            out_specs=vmem,
            scratch_shapes=[
                VMEM((rows, cols), BF16), VMEM((cols,), BF16),
                VMEM((8, local_rows, q_cols), BF16), VMEM(w_o.shape, BF16),
                VMEM((loads, cols, per_load * 2 * half), BF16), VMEM((loads, cols, per_load * 2 * half), BF16), VMEM((ring, per_load, 2, half, cols), BF16),
                VMEM((2, rows, cols), BF16), VMEM((2, rows, cols), BF16), VMEM((8, rows), F32), VMEM((8, 8, rows), F32),
                VMEM((rows, cols), BF16), VMEM((rows, cols), BF16), VMEM((rows, cols), F32),
            ] + [VMEM((chunks, 2, 2, 2, 2, 16, half // 2), BF16)] * 3 + [
                VMEM((chunks, 2, 2, 2, 16, half // 2), BF16), VMEM((chunks, 2, 2, 16, half // 2), BF16), VMEM((chunks, 2, 2, 2, 2, 16, half // 2), BF16),
                DMA((3,)), DMA((loads,)), DMA((loads,)), DMA((ring,)), DMA((8,)), DMA((8,)), DMA((2,)), DMA((2,)), DMA((8,)), DMA((8,)),
            ] + [DMA((chunks,))] * 12,
            compiler_params=pltpu.CompilerParams(collective_id=1, has_side_effects=True, vmem_limit_bytes=int(52.5 * 2 ** 20)),
            cost_estimate=pl.CostEstimate(flops=60_000_000_000, bytes_accessed=57_000_000, transcendentals=0),
        )(attn, hbm(x_in), hbm(gain_mlp), hbm(w_o), hbm(w_gate), hbm(w_up), hbm(w_down.reshape(loads, per_load, 2, half, cols)))
        return x_out, k_flat.reshape(k_cache.shape), v_flat.reshape(v_cache.shape)

    return jax.shard_map(local_layer, mesh=mesh, in_specs=in_specs, out_specs=out_specs, check_vma=False)
```

```python
import functools

import jax
import jax.numpy as jnp
from jax import lax
from jax.experimental import pallas as pl
from jax.experimental.pallas import tpu as pltpu
from jax.sharding import PartitionSpec as P

HEAD = 128
NORM_EPS = 1e-6
ROPE_THETA = 1000000.0
MESH = pl.DeviceIdType.MESH
F32 = jnp.float32
BF16 = jnp.bfloat16
VMEM = pltpu.VMEM
DMA = pltpu.SemaphoreType.DMA


def neighbours(mx):
    core = lax.rem(mx, 2)
    chip = mx // 2
    x_pos = lax.rem(chip, 2)
    y_pos = chip // 2
    others = (y_pos * 2 + (1 - x_pos), (1 - y_pos) * 2 + x_pos, (1 - y_pos) * 2 + (1 - x_pos))
    return core, chip, chip * 2 + (1 - core), others


def hbm(array):
    return pltpu.with_memory_space_constraint(array, pltpu.HBM)


def send(src, dst, send_sem, recv_sem, my, mx):
    copy = pltpu.make_async_remote_copy(src_ref=src, dst_ref=dst, send_sem=send_sem, recv_sem=recv_sem, device_id=(my, mx), device_id_type=MESH)
    copy.start()
    return copy


def drain(ref, sem):
    pltpu.make_async_copy(ref, ref, sem).wait()


def share_stat(square_sum, my, mx, stat_out, stat_in, send_sems, recv_sems, between=None):
    rows = square_sum.shape[0]
    turned = jnp.transpose(jnp.broadcast_to(square_sum, (rows, 128)))[0:8]
    stat_out[...] = turned
    copies = []
    for step in range(1, 8):
        peer = lax.rem(mx + step, 8)
        copies.append(send(stat_out, stat_in.at[mx], send_sems.at[step], recv_sems.at[step], my, peer))
    stat_in[mx] = turned
    if between is not None:
        between()
    for copy in copies:
        copy.wait()
    total = jnp.sum(stat_in[...], axis=0)
    return jnp.transpose(jnp.broadcast_to(total[0:1], (128, rows)))[:, 0:1]


def enter(my, mx, with_z, meanwhile=None):
    barrier = pltpu.get_barrier_semaphore()
    for step in range(1, 8):
        pl.semaphore_signal(barrier, inc=1, device_id=(my, lax.rem(mx + step, 8)), device_id_type=MESH)
    if with_z:
        pl.semaphore_signal(barrier, inc=1, device_id=(1 - my, mx), device_id_type=MESH)
    if meanwhile is not None:
        meanwhile()
    pl.semaphore_wait(barrier, 8 if with_z else 7)


def qkv_kernel(hidden, pieces, freq_ref, lens_hbm, x_hbm, gain_hbm, wq_hbm, wk_hbm, wv_hbm, bq_hbm, bk_hbm, bv_hbm, out_ref,
               lens_s, x_v, gain_v, wq_v, wk_v, wv_v, bq_v, bk_v, bv_v, cos_v, sin_v, part, pair_in, chip_in, stat_out, stat_in,
               w_sems, stat_send, stat_recv, pair_send, pair_recv, chip_send, chip_recv):
    my = lax.axis_index("my")
    mx = lax.axis_index("mx")
    core, chip, partner, others = neighbours(mx)
    loads = [pltpu.make_async_copy(src, dst, w_sems.at[n]) for n, (src, dst) in enumerate((
        (wq_hbm, wq_v), (wk_hbm, wk_v), (wv_hbm, wv_v), (x_hbm, x_v), (gain_hbm, gain_v), (lens_hbm, lens_s), (bq_hbm, bq_v), (bk_hbm, bk_v), (bv_hbm, bv_v)))]
    for n in (3, 4, 5, 0, 1, 2, 6, 7, 8):
        loads[n].start()
    enter(my, mx, False, loads[3].wait)
    x = x_v[...].astype(F32)
    square_sum = jnp.sum(x * x, axis=1, keepdims=True)

    def tables():
        loads[4].wait()
        loads[5].wait()
        rows = lens_s.shape[0]
        sub = lax.broadcasted_iota(jnp.int32, (rows, HEAD // 2), 0)
        position = jnp.zeros((rows, HEAD // 2), F32)
        for b in range(rows):
            position = jnp.where(sub == b, lens_s[b].astype(F32), position)
        angles = position * freq_ref[...][None, :]
        cos_half = jnp.cos(angles)
        sin_half = jnp.sin(angles)
        cos_v[...] = jnp.concatenate([cos_half, cos_half], axis=1)
        sin_v[...] = jnp.concatenate([-sin_half, sin_half], axis=1)
        for n in (0, 1, 2, 6, 7, 8):
            loads[n].wait()

    stat = share_stat(square_sum, my, mx, stat_out, stat_in, stat_send, stat_recv, tables)
    normed = (x * lax.rsqrt(stat / hidden + NORM_EPS) * gain_v[...].astype(F32)[None, :]).astype(BF16)
    weights = (wq_v, wk_v, wv_v)
    biases = (bq_v, bk_v, bv_v)
    copies = []
    pair_copies = []
    for n, (which, first, width, out_first) in enumerate(pieces):
        cols = pl.ds(out_first, width)
        product = jnp.dot(normed, weights[which][:, first:first + width], preferred_element_type=F32)
        part[:, :, :, cols] = product.reshape(4, 2, 8, width).astype(BF16)
        pair_copies.append(send(part.at[:, 1 - core, :, cols], pair_in.at[:, :, cols], pair_send.at[n], pair_recv.at[n], my, partner))
    for n, (which, first, width, out_first) in enumerate(pieces):
        cols = pl.ds(out_first, width)
        pair_copies[n].wait_recv()
        pair_in[:, :, cols] = (part[:, core, :, cols].astype(F32) + pair_in[:, :, cols].astype(F32)).astype(BF16)
        for k, other in enumerate(others):
            copies.append(send(pair_in.at[other, :, cols], chip_in.at[k, :, cols], chip_send.at[n, k], chip_recv.at[n, k], my, other * 2 + core))
    for n, (which, first, width, out_first) in enumerate(pieces):
        cols = pl.ds(out_first, width)
        total = pair_in[chip, :, cols].astype(F32)
        for k in range(3):
            copies[n * 3 + k].wait_recv()
            total = total + chip_in[k, :, cols].astype(F32)
        total = total + biases[which][first:first + width].astype(F32)[None, :]
        for h in range(0, width, HEAD):
            vals = total[:, h:h + HEAD]
            if which < 2:
                vals = vals * cos_v[...] + pltpu.roll(vals, HEAD // 2, 1) * sin_v[...]
            out_ref[:, out_first + h:out_first + h + HEAD] = vals
    for copy in pair_copies + copies:
        copy.wait_send()


def attend_kernel(heads, proj_ref, k_ref, v_ref, lens_hbm, ko_hbm, vo_hbm, attn_ref,
                  lens_s, q_s, k_s, v_s, o_s, k_win, v_win, lens_sem, out_sems, win_sems):
    rows, slots, _ = k_ref.shape
    q_cols = heads * HEAD
    kv_cols = (proj_ref.shape[1] - q_cols) // 2
    kv_heads = kv_cols // HEAD
    group = heads // kv_heads
    load_lens = pltpu.make_async_copy(lens_hbm, lens_s, lens_sem)
    load_lens.start()
    outs = []
    for b in range(rows):
        outs.append((pltpu.make_async_copy(k_ref.at[b], ko_hbm.at[b], out_sems.at[0, b]), pltpu.make_async_copy(v_ref.at[b], vo_hbm.at[b], out_sems.at[1, b])))
        for out in outs[b]:
            out.start()
    q_s[...] = jnp.zeros_like(q_s)
    for h in range(heads):
        q_s[:, h, :] = proj_ref[:, h * HEAD:(h + 1) * HEAD]
    for h in range(kv_heads):
        k_new = proj_ref[:, q_cols + h * HEAD:q_cols + (h + 1) * HEAD]
        v_new = proj_ref[:, q_cols + kv_cols + h * HEAD:q_cols + kv_cols + (h + 1) * HEAD]
        for r in range(16 // kv_heads):
            k_s[:, r * kv_heads + h, :] = k_new
            v_s[:, r * kv_heads + h, :] = v_new
    load_lens.wait()
    q_pad = q_s.shape[1]
    per_tile = 16 // kv_heads
    sub = lax.broadcasted_iota(jnp.int32, (16, HEAD), 0) // kv_heads
    row = lax.broadcasted_iota(jnp.int32, (q_pad, 1), 0)
    row_head = sum((row >= group * n).astype(jnp.int32) for n in range(1, kv_heads))
    col = lax.broadcasted_iota(jnp.int32, (q_pad, slots), 1)
    offset = jnp.where(lax.rem(col, kv_heads) == row_head, col // kv_heads, slots)
    new_col = lax.broadcasted_iota(jnp.int32, (q_pad, 16), 1)

    def window(b, position):
        base = pl.multiple_of(position // per_tile * 16, 16)
        at_slot = sub == lax.rem(position, per_tile)
        for src, new, win in ((k_ref, k_s, k_win), (v_ref, v_s, v_win)):
            win[b] = jnp.where(at_slot, new[b], src[b, pl.ds(base, 16), :].astype(F32)).astype(BF16)

    def one_row(b):
        position = lens_s[b]
        if b < rows - 1:
            window(b, position)
        query = q_s[b].astype(BF16)
        scores = lax.dot_general(query, k_ref[b], (((1,), (1,)), ((), ())), preferred_element_type=F32) * HEAD ** -0.5
        scores = jnp.where(offset < position, scores, -jnp.inf)
        new_scores = lax.dot_general(query, k_s[b].astype(BF16), (((1,), (1,)), ((), ())), preferred_element_type=F32) * HEAD ** -0.5
        new_scores = jnp.where(new_col == row_head, new_scores, -jnp.inf)
        top = jnp.maximum(jnp.max(scores, axis=1, keepdims=True), jnp.max(new_scores, axis=1, keepdims=True))
        weights = jnp.exp(scores - top)
        new_weights = jnp.exp(new_scores - top)
        weight_sum = jnp.sum(weights, axis=1, keepdims=True) + jnp.sum(new_weights, axis=1, keepdims=True)
        weighted = jnp.dot(weights.astype(BF16), v_ref[b], preferred_element_type=F32)
        weighted = weighted + jnp.dot(new_weights.astype(BF16), v_s[b].astype(BF16), preferred_element_type=F32)
        o_s[b] = weighted / weight_sum

    def fix(b):
        base = pl.multiple_of(lens_s[b] // per_tile * 16, 16)
        return [pltpu.make_async_copy(win.at[b], hbm_out.at[b, pl.ds(base, 16), :], win_sems.at[n, b]) for n, (win, hbm_out) in enumerate(((k_win, ko_hbm), (v_win, vo_hbm)))]

    for b in range(rows - 1):
        one_row(b)
    window(rows - 1, lens_s[rows - 1])
    for b in range(rows):
        for out, win in zip(outs[b], fix(b)):
            out.wait()
            win.start()
    one_row(rows - 1)
    for h in range(heads):
        attn_ref[:, h * HEAD:(h + 1) * HEAD] = o_s[:, h, :].astype(BF16)
    for b in range(rows):
        for win in fix(b):
            win.wait()


def mlp_kernel(hidden, chunks, per_load, lags, attn_ref, x_hbm, gain_hbm, wo_hbm, wg_hbm, wu_hbm, wd_hbm, out_ref,
               x_v, gain_v, attn_all, wo_v, wg_v, wu_v, wd_v, z_out, z_in, stat_out, stat_in, h_v, m_v, acc, mine, theirs, pair_in, hop_in, fin_in, act,
               in_sems, wg_sems, wu_sems, wd_sems, ag_send, ag_recv, z_send, z_recv, stat_send, stat_recv,
               pair_send, pair_recv, hop_send, hop_recv, fin_send, fin_recv, near_send, near_recv, far_send, far_recv, fwd_send, fwd_recv):
    my = lax.axis_index("my")
    mx = lax.axis_index("mx")
    core, chip, partner, others = neighbours(mx)
    x_pos = lax.rem(chip, 2)
    y_pos = chip // 2
    x_peer = others[0] * 2 + core
    y_peer = others[1] * 2 + core
    half = 2 * act.shape[6]
    loads = chunks // per_load
    load_cols = per_load * 2 * half
    ring = wg_v.shape[0]

    firsts = [pltpu.make_async_copy(src, dst, in_sems.at[n]) for n, (src, dst) in enumerate(((wo_hbm, wo_v), (x_hbm, x_v), (gain_hbm, gain_v)))]
    for first in firsts:
        first.start()

    def load_gate(n):
        cols = pl.ds(pl.multiple_of(n * load_cols, 128), load_cols)
        slot = lax.rem(n, ring)
        return pltpu.make_async_copy(wg_hbm.at[:, cols], wg_v.at[slot], wg_sems.at[slot]), pltpu.make_async_copy(wu_hbm.at[:, cols], wu_v.at[slot], wu_sems.at[slot])

    def load_down(n):
        return pltpu.make_async_copy(wd_hbm.at[n], wd_v.at[n], wd_sems.at[n])

    @pl.loop(0, ring)
    def _(n):
        for load in load_gate(n):
            load.start()

    @pl.loop(0, loads)
    def _(n):
        load_down(n).start()

    enter(my, mx, True)

    copies = []
    for step in range(1, 8):
        peer = lax.rem(mx + step, 8)
        copies.append(send(attn_ref, attn_all.at[mx], ag_send.at[step], ag_recv.at[step], my, peer))
    attn_all[mx] = attn_ref[...]
    for first in firsts:
        first.wait()
    for copy in copies:
        copy.wait()
    rows = x_v.shape[0]
    attn = attn_all[...].reshape(rows, attn_ref.shape[1])
    z_out[0] = jnp.dot(attn, wo_v[...], preferred_element_type=F32).astype(BF16)
    z_copy = send(z_out.at[0], z_in.at[0], z_send.at[0], z_recv.at[0], 1 - my, mx)
    z_copy.wait()
    mid = (x_v[...].astype(F32) + (z_out[0].astype(F32) + z_in[0].astype(F32))).astype(BF16)
    m_v[...] = mid
    mid = mid.astype(F32)
    stat = share_stat(jnp.sum(mid * mid, axis=1, keepdims=True), my, mx, stat_out, stat_in, stat_send, stat_recv)
    h_v[...] = (mid * lax.rsqrt(stat / hidden + NORM_EPS) * gain_v[...].astype(F32)[None, :]).astype(BF16)
    acc[...] = jnp.zeros_like(acc)

    def multiply(k):
        n = k // per_load
        slot = lax.rem(n, ring)
        step = lax.rem(k, per_load)

        @pl.when(step == 0)
        def _():
            for load in load_gate(n):
                load.wait()

        h = h_v[...]

        def products(part, dest):
            cols = pl.ds(pl.multiple_of(step * (2 * half) + part * half, 128), half)
            for which, weights in ((0, wg_v), (1, wu_v)):
                out = jnp.dot(h, weights[slot, :, cols], preferred_element_type=F32).astype(BF16)
                for way in range(2):
                    dest[k, way, :, :, which] = out[:, way * half // 2:(way + 1) * half // 2].reshape(2, 2, 16, half // 2)

        products(1 - core, theirs)
        send(theirs.at[k], pair_in.at[k], pair_send.at[k], pair_recv.at[k], my, partner)
        products(core, mine)

        @pl.when(jnp.logical_and(step == per_load - 1, n + ring < loads))
        def _():
            for load in load_gate(n + ring):
                load.start()

    def scatter(k):
        drain(pair_in.at[k], pair_recv.at[k])
        pair_in[k] = (mine[k].astype(F32) + pair_in[k].astype(F32)).astype(BF16)
        send(pair_in.at[k, 0, :, 1 - x_pos], hop_in.at[k, 0], hop_send.at[k], hop_recv.at[k], my, x_peer)
        send(pair_in.at[k, 1, 1 - y_pos], hop_in.at[k, 1], hop_send.at[k], hop_recv.at[k], my, y_peer)

    def combine(k):
        drain(hop_in.at[k], hop_recv.at[k])
        hop_in[k, 0] = (pair_in[k, 0, :, x_pos].astype(F32) + hop_in[k, 0].astype(F32)).astype(BF16)
        hop_in[k, 1] = (pair_in[k, 1, y_pos].astype(F32) + hop_in[k, 1].astype(F32)).astype(BF16)
        send(hop_in.at[k, 0, 1 - y_pos], fin_in.at[k, 0], fin_send.at[k], fin_recv.at[k], my, y_peer)
        send(hop_in.at[k, 1, 1 - x_pos], fin_in.at[k, 1], fin_send.at[k], fin_recv.at[k], my, x_peer)

    def activate(k):
        drain(fin_in.at[k], fin_recv.at[k])
        for way, own in ((0, y_pos), (1, x_pos)):
            total = hop_in[k, way, own].astype(F32) + fin_in[k, way].astype(F32)
            gate = total[0]
            act[k, core, way, y_pos, x_pos] = (gate * jax.nn.sigmoid(gate) * total[1]).astype(BF16)
        for way, peer in ((0, y_peer), (1, x_peer)):
            block = act.at[k, core, way, y_pos, x_pos]
            send(block, block, near_send.at[k], near_recv.at[k], my, peer)
        both = act.at[k, core, :, y_pos, x_pos]
        send(both, both, fwd_send.at[k], fwd_recv.at[k], my, partner)

    def gather(k):
        drain(act.at[k, core, 0, 0], near_recv.at[k])
        for block, peer in ((act.at[k, core, 0, :, x_pos], x_peer), (act.at[k, core, 1, y_pos], y_peer)):
            send(block, block, far_send.at[k], far_recv.at[k], my, peer)
        for block in (act.at[k, core, 0, 1 - y_pos, x_pos], act.at[k, core, 1, y_pos, 1 - x_pos]):
            send(block, block, fwd_send.at[k], fwd_recv.at[k], my, partner)

    def forward(k):
        drain(act.at[k, core, 0], far_recv.at[k])
        for block in (act.at[k, core, 0, :, 1 - x_pos], act.at[k, core, 1, 1 - y_pos]):
            send(block, block, fwd_send.at[k], fwd_recv.at[k], my, partner)

    def contract(k):
        n = k // per_load
        step = lax.rem(k, per_load)

        @pl.when(step == 0)
        def _():
            load_down(n).wait()

        drain(act.at[k, 1 - core], fwd_recv.at[k])
        total = acc[...]
        for part in range(2):
            lhs = jnp.concatenate([act[k, part, way].reshape(rows, half // 2) for way in range(2)], axis=1)
            total = total + jnp.dot(lhs, wd_v[n, step, part], preferred_element_type=F32)
        acc[...] = total

    stages = tuple(zip((contract, forward, gather, activate, combine, scatter, multiply), lags))

    @pl.loop(0, chunks + lags[0])
    def _(t):
        for stage, lag in stages:
            @pl.when(jnp.logical_and(t >= lag, t < chunks + lag))
            def _():
                stage(t - lag)

    z_out[1] = acc[...].astype(BF16)
    z_copy = send(z_out.at[1], z_in.at[1], z_send.at[1], z_recv.at[1], 1 - my, mx)
    z_copy.wait()
    out_ref[...] = (m_v[...].astype(F32) + (z_out[1].astype(F32) + z_in[1].astype(F32))).astype(BF16)

    @pl.loop(0, chunks)
    def _(k):
        drain(theirs.at[k], pair_send.at[k])
        drain(hop_in.at[k], hop_send.at[k])
        drain(fin_in.at[k], fin_send.at[k])
        drain(act.at[k, core, 0, 0], near_send.at[k])
        drain(act.at[k, core, 0], far_send.at[k])
        drain(act.at[k, core], fwd_send.at[k])


def solution(mesh):
    mx_size = mesh.shape["mx"]
    act_spec = P(None, "mx")
    cache_spec = P("mx", None, "my", None)
    in_specs = (act_spec, P("mx"), P("mx"), P("mx"), P("mx", "my"), P("my"), P("mx", "my"), P("my"), P("mx", "my"), P("my"), P("my", "mx"), P("mx", "my"), P("mx", "my"), P("my", "mx"), cache_spec, cache_spec)
    out_specs = (act_spec, cache_spec, cache_spec)
    vmem = pl.BlockSpec(memory_space=pltpu.VMEM)
    anywhere = pl.BlockSpec(memory_space=pl.ANY)

    def local_layer(x_in, seq_lens, gain_attn, gain_mlp, w_q, b_q, w_k, b_k, w_v, b_v, w_o, w_gate, w_up, w_down, k_cache, v_cache):
        rows, cols = x_in.shape
        hidden = cols * mx_size
        q_cols = w_q.shape[1]
        kv_cols = w_k.shape[1]
        heads = q_cols // HEAD
        kv_heads = kv_cols // HEAD
        local_rows = rows // mx_size
        qkv_cols = q_cols + 2 * kv_cols
        pieces = ((0, 0, q_cols // 2, 0), (0, q_cols // 2, q_cols // 2, q_cols // 2), (1, 0, kv_cols, q_cols), (2, 0, kv_cols, q_cols + kv_cols))
        inv_freq = ROPE_THETA ** (-2.0 * jnp.arange(HEAD // 2, dtype=F32) / HEAD)

        projected = pl.pallas_call(
            functools.partial(qkv_kernel, hidden, pieces),
            name="qkv",
            out_shape=jax.ShapeDtypeStruct((local_rows, qkv_cols), F32),
            in_specs=[vmem] + [anywhere] * 9,
            out_specs=vmem,
            scratch_shapes=[
                pltpu.SMEM((local_rows,), jnp.int32), VMEM((rows, cols), BF16), VMEM((cols,), BF16),
                VMEM(w_q.shape, BF16), VMEM(w_k.shape, BF16), VMEM(w_v.shape, BF16), VMEM(b_q.shape, BF16), VMEM(b_k.shape, BF16), VMEM(b_v.shape, BF16),
                VMEM((local_rows, HEAD), F32), VMEM((local_rows, HEAD), F32),
                VMEM((4, 2, local_rows, qkv_cols), BF16), VMEM((4, local_rows, qkv_cols), BF16), VMEM((3, local_rows, qkv_cols), BF16),
                VMEM((8, rows), F32), VMEM((8, 8, rows), F32),
                DMA((9,)), DMA((8,)), DMA((8,)), DMA((4,)), DMA((4,)), DMA((4, 3)), DMA((4, 3)),
            ],
            compiler_params=pltpu.CompilerParams(collective_id=0, has_side_effects=True, vmem_limit_bytes=16 * 2 ** 20),
            cost_estimate=pl.CostEstimate(flops=40_000_000_000, bytes_accessed=4_600_000, transcendentals=0),
        )(inv_freq, hbm(seq_lens), hbm(x_in), hbm(gain_attn), hbm(w_q), hbm(w_k), hbm(w_v), hbm(b_q), hbm(b_k), hbm(b_v))

        slots = k_cache.shape[1] * kv_heads
        flat = (local_rows, slots, HEAD)
        padded = (heads + 7) // 8 * 8
        k_flat, v_flat, attn = pl.pallas_call(
            functools.partial(attend_kernel, heads),
            name="attend",
            out_shape=(jax.ShapeDtypeStruct(flat, BF16), jax.ShapeDtypeStruct(flat, BF16), jax.ShapeDtypeStruct((local_rows, q_cols), BF16)),
            in_specs=[vmem] * 3 + [anywhere],
            out_specs=(anywhere, anywhere, vmem),
            scratch_shapes=[
                pltpu.SMEM((local_rows,), jnp.int32),
                VMEM((local_rows, padded, HEAD), F32), VMEM((local_rows, 16, HEAD), F32), VMEM((local_rows, 16, HEAD), F32), VMEM((local_rows, padded, HEAD), F32),
                VMEM((local_rows, 16, HEAD), BF16), VMEM((local_rows, 16, HEAD), BF16),
                DMA, DMA((2, local_rows)), DMA((2, local_rows)),
            ],
            compiler_params=pltpu.CompilerParams(vmem_limit_bytes=26 * 2 ** 20),
            cost_estimate=pl.CostEstimate(flops=20_000_000_000, bytes_accessed=17_000_000, transcendentals=0),
        )(projected, pltpu.with_memory_space_constraint(k_cache.reshape(flat), VMEM), pltpu.with_memory_space_constraint(v_cache.reshape(flat), VMEM), hbm(seq_lens))

        ff_cols = w_gate.shape[1]
        half = 768
        chunks = ff_cols // (2 * half)
        per_load = 1
        ring = 6
        loads = chunks // per_load
        lags = (20, 17, 13, 9, 5, 2, 0)
        x_out = pl.pallas_call(
            functools.partial(mlp_kernel, hidden, chunks, per_load, lags),
            name="mlp",
            out_shape=jax.ShapeDtypeStruct((rows, cols), BF16),
            in_specs=[vmem] + [anywhere] * 6,
            out_specs=vmem,
            scratch_shapes=[
                VMEM((rows, cols), BF16), VMEM((cols,), BF16),
                VMEM((8, local_rows, q_cols), BF16), VMEM(w_o.shape, BF16),
                VMEM((ring, cols, per_load * 2 * half), BF16), VMEM((ring, cols, per_load * 2 * half), BF16), VMEM((loads, per_load, 2, half, cols), BF16),
                VMEM((2, rows, cols), BF16), VMEM((2, rows, cols), BF16), VMEM((8, rows), F32), VMEM((8, 8, rows), F32),
                VMEM((rows, cols), BF16), VMEM((rows, cols), BF16), VMEM((rows, cols), F32),
            ] + [VMEM((chunks, 2, 2, 2, 2, 16, half // 2), BF16)] * 3 + [
                VMEM((chunks, 2, 2, 2, 16, half // 2), BF16), VMEM((chunks, 2, 2, 16, half // 2), BF16), VMEM((chunks, 2, 2, 2, 2, 16, half // 2), BF16),
                DMA((3,)), DMA((ring,)), DMA((ring,)), DMA((loads,)), DMA((8,)), DMA((8,)), DMA((2,)), DMA((2,)), DMA((8,)), DMA((8,)),
            ] + [DMA((chunks,))] * 12,
            compiler_params=pltpu.CompilerParams(collective_id=1, has_side_effects=True, vmem_limit_bytes=int(52.5 * 2 ** 20)),
            cost_estimate=pl.CostEstimate(flops=60_000_000_000, bytes_accessed=57_000_000, transcendentals=0),
        )(attn, hbm(x_in), hbm(gain_mlp), hbm(w_o), hbm(w_gate), hbm(w_up), hbm(w_down.reshape(loads, per_load, 2, half, cols)))
        return x_out, k_flat.reshape(k_cache.shape), v_flat.reshape(v_cache.shape)

    return jax.shard_map(local_layer, mesh=mesh, in_specs=in_specs, out_specs=out_specs, check_vma=False)
```

```python
import functools

import jax
import jax.numpy as jnp
from jax import lax
from jax.experimental import pallas as pl
from jax.experimental.pallas import tpu as pltpu
from jax.sharding import PartitionSpec as P

HEAD = 128
NORM_EPS = 1e-6
ROPE_THETA = 1000000.0
MESH = pl.DeviceIdType.MESH
F32 = jnp.float32
BF16 = jnp.bfloat16
VMEM = pltpu.VMEM
DMA = pltpu.SemaphoreType.DMA


def neighbours(mx):
    core = lax.rem(mx, 2)
    chip = mx // 2
    x_pos = lax.rem(chip, 2)
    y_pos = chip // 2
    others = (y_pos * 2 + (1 - x_pos), (1 - y_pos) * 2 + x_pos, (1 - y_pos) * 2 + (1 - x_pos))
    return core, chip, chip * 2 + (1 - core), others


def far_first(mx):
    core, chip, partner, others = neighbours(mx)
    return [other * 2 + c for other in (others[2], others[0], others[1]) for c in (core, 1 - core)] + [partner]


def hbm(array):
    return pltpu.with_memory_space_constraint(array, pltpu.HBM)


def send(src, dst, send_sem, recv_sem, my, mx):
    copy = pltpu.make_async_remote_copy(src_ref=src, dst_ref=dst, send_sem=send_sem, recv_sem=recv_sem, device_id=(my, mx), device_id_type=MESH)
    copy.start()
    return copy


def drain(ref, sem):
    pltpu.make_async_copy(ref, ref, sem).wait()


def share_stat(square_sum, my, mx, stat_out, stat_in, send_sems, recv_sems, between=None):
    rows = square_sum.shape[0]
    turned = jnp.transpose(jnp.broadcast_to(square_sum, (rows, 128)))[0:8]
    stat_out[...] = turned
    copies = []
    for step, peer in enumerate(far_first(mx)):
        copies.append(send(stat_out, stat_in.at[mx], send_sems.at[step], recv_sems.at[step], my, peer))
    stat_in[mx] = turned
    if between is not None:
        between()
    for copy in copies:
        copy.wait()
    total = jnp.sum(stat_in[...], axis=0)
    return jnp.transpose(jnp.broadcast_to(total[0:1], (128, rows)))[:, 0:1]


def enter(my, mx, with_z, meanwhile=None):
    barrier = pltpu.get_barrier_semaphore()
    for step in range(1, 8):
        pl.semaphore_signal(barrier, inc=1, device_id=(my, lax.rem(mx + step, 8)), device_id_type=MESH)
    if with_z:
        pl.semaphore_signal(barrier, inc=1, device_id=(1 - my, mx), device_id_type=MESH)
    if meanwhile is not None:
        meanwhile()
    pl.semaphore_wait(barrier, 8 if with_z else 7)


def qkv_kernel(hidden, pieces, freq_ref, lens_hbm, x_hbm, gain_hbm, wq_hbm, wk_hbm, wv_hbm, bq_hbm, bk_hbm, bv_hbm, out_ref,
               lens_s, x_v, gain_v, wq_v, wk_v, wv_v, bq_v, bk_v, bv_v, cos_v, sin_v, part, pair_in, chip_in, direct_in, stat_out, stat_in,
               w_sems, stat_send, stat_recv, pair_send, pair_recv, chip_send, chip_recv, direct_send, direct_recv):
    my = lax.axis_index("my")
    mx = lax.axis_index("mx")
    core, chip, partner, others = neighbours(mx)
    loads = [pltpu.make_async_copy(src, dst, w_sems.at[n]) for n, (src, dst) in enumerate((
        (wq_hbm, wq_v), (wk_hbm, wk_v), (wv_hbm, wv_v), (x_hbm, x_v), (gain_hbm, gain_v), (lens_hbm, lens_s), (bq_hbm, bq_v), (bk_hbm, bk_v), (bv_hbm, bv_v)))]
    loads[3].start()

    def meanwhile():
        for n in (4, 5, 0, 1, 2, 6, 7, 8):
            loads[n].start()
        loads[3].wait()

    enter(my, mx, False, meanwhile)
    x = x_v[...].astype(F32)
    square_sum = jnp.sum(x * x, axis=1, keepdims=True)

    def tables():
        loads[4].wait()
        loads[5].wait()
        rows = lens_s.shape[0]
        sub = lax.broadcasted_iota(jnp.int32, (rows, HEAD // 2), 0)
        position = jnp.zeros((rows, HEAD // 2), F32)
        for b in range(rows):
            position = jnp.where(sub == b, lens_s[b].astype(F32), position)
        angles = position * freq_ref[...][None, :]
        cos_half = jnp.cos(angles)
        sin_half = jnp.sin(angles)
        cos_v[...] = jnp.concatenate([cos_half, cos_half], axis=1)
        sin_v[...] = jnp.concatenate([-sin_half, sin_half], axis=1)
        for n in (0, 1, 2, 6, 7, 8):
            loads[n].wait()

    stat = share_stat(square_sum, my, mx, stat_out, stat_in, stat_send, stat_recv, tables)
    normed = (x * lax.rsqrt(stat / hidden + NORM_EPS) * gain_v[...].astype(F32)[None, :]).astype(BF16)
    weights = (wq_v, wk_v, wv_v)
    biases = (bq_v, bk_v, bv_v)
    copies = []
    pair_copies = []
    direct = []
    for n, (which, first, width, out_first) in enumerate(pieces):
        cols = pl.ds(out_first, width)
        product = jnp.dot(normed, weights[which][:, first:first + width], preferred_element_type=F32)
        part[:, :, :, cols] = product.reshape(4, 2, 8, width).astype(BF16)
        if n == 0:
            for k, peer in enumerate(far_first(mx)):
                direct.append(send(part.at[peer // 2, lax.rem(peer, 2), :, cols], direct_in.at[k], direct_send.at[k], direct_recv.at[k], my, peer))
        else:
            pair_copies.append(send(part.at[:, 1 - core, :, cols], pair_in.at[:, :, cols], pair_send.at[n - 1], pair_recv.at[n - 1], my, partner))
    for n, (which, first, width, out_first) in enumerate(pieces[1:]):
        cols = pl.ds(out_first, width)
        pair_copies[n].wait_recv()
        pair_in[:, :, cols] = (part[:, core, :, cols].astype(F32) + pair_in[:, :, cols].astype(F32)).astype(BF16)
        for k, other in enumerate(others):
            copies.append(send(pair_in.at[other, :, cols], chip_in.at[k, :, cols], chip_send.at[n, k], chip_recv.at[n, k], my, other * 2 + core))
    for n, (which, first, width, out_first) in enumerate(pieces):
        cols = pl.ds(out_first, width)
        if n == 0:
            total = part[chip, core, :, cols].astype(F32)
            for k in range(7):
                direct[k].wait_recv()
                total = total + direct_in[k].astype(F32)
        else:
            total = pair_in[chip, :, cols].astype(F32)
            for k in range(3):
                copies[(n - 1) * 3 + k].wait_recv()
                total = total + chip_in[k, :, cols].astype(F32)
        total = total + biases[which][first:first + width].astype(F32)[None, :]
        for h in range(0, width, HEAD):
            vals = total[:, h:h + HEAD]
            if which < 2:
                vals = vals * cos_v[...] + pltpu.roll(vals, HEAD // 2, 1) * sin_v[...]
            out_ref[:, out_first + h:out_first + h + HEAD] = vals
    for copy in direct + pair_copies + copies:
        copy.wait_send()


def attend_kernel(heads, proj_ref, k_ref, v_ref, lens_hbm, ko_hbm, vo_hbm, attn_ref,
                  lens_s, q_s, k_s, v_s, o_s, k_win, v_win, lens_sem, out_sems, win_sems):
    rows, slots, _ = k_ref.shape
    q_cols = heads * HEAD
    kv_cols = (proj_ref.shape[1] - q_cols) // 2
    kv_heads = kv_cols // HEAD
    group = heads // kv_heads
    load_lens = pltpu.make_async_copy(lens_hbm, lens_s, lens_sem)
    load_lens.start()
    outs = []
    for b in range(rows):
        outs.append((pltpu.make_async_copy(k_ref.at[b], ko_hbm.at[b], out_sems.at[0, b]), pltpu.make_async_copy(v_ref.at[b], vo_hbm.at[b], out_sems.at[1, b])))
        for out in outs[b]:
            out.start()
    q_s[...] = jnp.zeros_like(q_s)
    for h in range(heads):
        q_s[:, h, :] = proj_ref[:, h * HEAD:(h + 1) * HEAD]
    for h in range(kv_heads):
        k_new = proj_ref[:, q_cols + h * HEAD:q_cols + (h + 1) * HEAD]
        v_new = proj_ref[:, q_cols + kv_cols + h * HEAD:q_cols + kv_cols + (h + 1) * HEAD]
        for r in range(16 // kv_heads):
            k_s[:, r * kv_heads + h, :] = k_new
            v_s[:, r * kv_heads + h, :] = v_new
    load_lens.wait()
    q_pad = q_s.shape[1]
    per_tile = 16 // kv_heads
    sub = lax.broadcasted_iota(jnp.int32, (16, HEAD), 0) // kv_heads
    row = lax.broadcasted_iota(jnp.int32, (q_pad, 1), 0)
    row_head = sum((row >= group * n).astype(jnp.int32) for n in range(1, kv_heads))
    col = lax.broadcasted_iota(jnp.int32, (q_pad, slots), 1)
    offset = jnp.where(lax.rem(col, kv_heads) == row_head, col // kv_heads, slots)
    new_col = lax.broadcasted_iota(jnp.int32, (q_pad, 16), 1)

    def window(b, position):
        base = pl.multiple_of(position // per_tile * 16, 16)
        at_slot = sub == lax.rem(position, per_tile)
        for src, new, win in ((k_ref, k_s, k_win), (v_ref, v_s, v_win)):
            win[b] = jnp.where(at_slot, new[b], src[b, pl.ds(base, 16), :].astype(F32)).astype(BF16)

    def one_row(b):
        position = lens_s[b]
        if b < rows - 1:
            window(b, position)
        query = q_s[b].astype(BF16)
        scores = lax.dot_general(query, k_ref[b], (((1,), (1,)), ((), ())), preferred_element_type=F32) * HEAD ** -0.5
        scores = jnp.where(offset < position, scores, -jnp.inf)
        new_scores = lax.dot_general(query, k_s[b].astype(BF16), (((1,), (1,)), ((), ())), preferred_element_type=F32) * HEAD ** -0.5
        new_scores = jnp.where(new_col == row_head, new_scores, -jnp.inf)
        top = jnp.maximum(jnp.max(scores, axis=1, keepdims=True), jnp.max(new_scores, axis=1, keepdims=True))
        weights = jnp.exp(scores - top)
        new_weights = jnp.exp(new_scores - top)
        weight_sum = jnp.sum(weights, axis=1, keepdims=True) + jnp.sum(new_weights, axis=1, keepdims=True)
        weighted = jnp.dot(weights.astype(BF16), v_ref[b], preferred_element_type=F32)
        weighted = weighted + jnp.dot(new_weights.astype(BF16), v_s[b].astype(BF16), preferred_element_type=F32)
        o_s[b] = weighted / weight_sum

    def fix(b):
        base = pl.multiple_of(lens_s[b] // per_tile * 16, 16)
        return [pltpu.make_async_copy(win.at[b], hbm_out.at[b, pl.ds(base, 16), :], win_sems.at[n, b]) for n, (win, hbm_out) in enumerate(((k_win, ko_hbm), (v_win, vo_hbm)))]

    for b in range(rows - 1):
        one_row(b)
    window(rows - 1, lens_s[rows - 1])
    for b in range(rows):
        for out, win in zip(outs[b], fix(b)):
            out.wait()
            win.start()
    one_row(rows - 1)
    for h in range(heads):
        attn_ref[:, h * HEAD:(h + 1) * HEAD] = o_s[:, h, :].astype(BF16)
    for b in range(rows):
        for win in fix(b):
            win.wait()


def mlp_kernel(hidden, chunks, per_load, lags, attn_ref, x_hbm, gain_hbm, wo_hbm, wg_hbm, wu_hbm, wd_hbm, out_ref,
               x_v, gain_v, attn_all, wo_v, wg_v, wu_v, wd_v, z_out, z_in, stat_out, stat_in, h_v, m_v, acc, mine, theirs, pair_in, hop_in, fin_in, act,
               in_sems, wg_sems, wu_sems, wd_sems, ag_send, ag_recv, z_send, z_recv, stat_send, stat_recv,
               pair_send, pair_recv, hop_send, hop_recv, fin_send, fin_recv, near_send, near_recv, far_send, far_recv, fwd_send, fwd_recv):
    my = lax.axis_index("my")
    mx = lax.axis_index("mx")
    core, chip, partner, others = neighbours(mx)
    x_pos = lax.rem(chip, 2)
    y_pos = chip // 2
    x_peer = others[0] * 2 + core
    y_peer = others[1] * 2 + core
    x_across = others[0] * 2 + (1 - core)
    y_across = others[1] * 2 + (1 - core)
    straight = chunks - 1
    half = 2 * act.shape[6]
    loads = chunks // per_load
    load_cols = per_load * 2 * half
    ring = wg_v.shape[0]

    def load_gate(n):
        cols = pl.ds(pl.multiple_of(n * load_cols, 128), load_cols)
        slot = lax.rem(n, ring)
        return pltpu.make_async_copy(wg_hbm.at[:, cols], wg_v.at[slot], wg_sems.at[slot]), pltpu.make_async_copy(wu_hbm.at[:, cols], wu_v.at[slot], wu_sems.at[slot])

    def load_down(n):
        return pltpu.make_async_copy(wd_hbm.at[n], wd_v.at[n], wd_sems.at[n])

    firsts = [pltpu.make_async_copy(src, dst, in_sems.at[n]) for n, (src, dst) in enumerate(((wo_hbm, wo_v), (x_hbm, x_v), (gain_hbm, gain_v)))]

    def meanwhile():
        for first in firsts:
            first.start()

        @pl.loop(0, ring)
        def _(n):
            for load in load_gate(n):
                load.start()

        @pl.loop(0, loads)
        def _(n):
            load_down(n).start()

        attn_all[mx] = attn_ref[...]
        acc[...] = jnp.zeros_like(acc)

    enter(my, mx, True, meanwhile)

    copies = []
    for step, peer in enumerate(far_first(mx)):
        copies.append(send(attn_ref, attn_all.at[mx], ag_send.at[step], ag_recv.at[step], my, peer))
    for first in firsts:
        first.wait()
    for copy in copies:
        copy.wait()
    rows = x_v.shape[0]
    attn = attn_all[...].reshape(rows, attn_ref.shape[1])
    z_parts = (pl.ds(0, 384), pl.ds(384, x_v.shape[1] - 384))
    z_copies = []
    for n, part in enumerate(z_parts):
        z_out[0, :, part] = jnp.dot(attn, wo_v[:, part], preferred_element_type=F32).astype(BF16)
        z_copies.append(send(z_out.at[0, :, part], z_in.at[0, :, part], z_send.at[n], z_recv.at[n], 1 - my, mx))
    for z_copy in z_copies:
        z_copy.wait()
    mid = (x_v[...].astype(F32) + (z_out[0].astype(F32) + z_in[0].astype(F32))).astype(BF16)
    m_v[...] = mid
    mid = mid.astype(F32)
    stat = share_stat(jnp.sum(mid * mid, axis=1, keepdims=True), my, mx, stat_out, stat_in, stat_send, stat_recv)
    h_v[...] = (mid * lax.rsqrt(stat / hidden + NORM_EPS) * gain_v[...].astype(F32)[None, :]).astype(BF16)

    def multiply(k):
        n = k // per_load
        slot = lax.rem(n, ring)
        step = lax.rem(k, per_load)

        @pl.when(step == 0)
        def _():
            for load in load_gate(n):
                load.wait()

        h = h_v[...]

        def products(part, dest):
            cols = pl.ds(pl.multiple_of(step * (2 * half) + part * half, 128), half)
            for which, weights in ((0, wg_v), (1, wu_v)):
                out = jnp.dot(h, weights[slot, :, cols], preferred_element_type=F32).astype(BF16)
                for way in range(2):
                    dest[k, way, :, :, which] = out[:, way * half // 2:(way + 1) * half // 2].reshape(2, 2, 16, half // 2)

        products(1 - core, theirs)
        send(theirs.at[k], pair_in.at[k], pair_send.at[k], pair_recv.at[k], my, partner)
        products(core, mine)

        @pl.when(jnp.logical_and(step == per_load - 1, n + ring < loads))
        def _():
            for load in load_gate(n + ring):
                load.start()

    def scatter(k):
        drain(pair_in.at[k], pair_recv.at[k])
        pair_in[k] = (mine[k].astype(F32) + pair_in[k].astype(F32)).astype(BF16)
        send(pair_in.at[k, 0, :, 1 - x_pos], hop_in.at[k, 0], hop_send.at[k], hop_recv.at[k], my, x_peer)
        send(pair_in.at[k, 1, 1 - y_pos], hop_in.at[k, 1], hop_send.at[k], hop_recv.at[k], my, y_peer)

    def combine(k):
        drain(hop_in.at[k], hop_recv.at[k])
        hop_in[k, 0] = (pair_in[k, 0, :, x_pos].astype(F32) + hop_in[k, 0].astype(F32)).astype(BF16)
        hop_in[k, 1] = (pair_in[k, 1, y_pos].astype(F32) + hop_in[k, 1].astype(F32)).astype(BF16)
        send(hop_in.at[k, 0, 1 - y_pos], fin_in.at[k, 0], fin_send.at[k], fin_recv.at[k], my, y_peer)
        send(hop_in.at[k, 1, 1 - x_pos], fin_in.at[k, 1], fin_send.at[k], fin_recv.at[k], my, x_peer)

    def activate(k):
        drain(fin_in.at[k], fin_recv.at[k])
        for way, own in ((0, y_pos), (1, x_pos)):
            total = hop_in[k, way, own].astype(F32) + fin_in[k, way].astype(F32)
            gate = total[0]
            act[k, core, way, y_pos, x_pos] = (gate * jax.nn.sigmoid(gate) * total[1]).astype(BF16)
        for way, peer in ((0, y_peer), (1, x_peer)):
            block = act.at[k, core, way, y_pos, x_pos]
            send(block, block, near_send.at[k], near_recv.at[k], my, peer)
        both = act.at[k, core, :, y_pos, x_pos]
        send(both, both, fwd_send.at[k], fwd_recv.at[k], my, partner)

    def gather(k):
        drain(act.at[k, core, 0, 0], near_recv.at[k])
        for block, peer in ((act.at[k, core, 0, :, x_pos], x_peer), (act.at[k, core, 1, y_pos], y_peer)):
            send(block, block, far_send.at[k], far_recv.at[k], my, peer)
        for block in (act.at[k, core, 0, 1 - y_pos, x_pos], act.at[k, core, 1, y_pos, 1 - x_pos]):
            send(block, block, fwd_send.at[k], fwd_recv.at[k], my, partner)

        @pl.when(k >= straight)
        def _():
            for block, peer in ((act.at[k, core, 0, :, x_pos], x_across), (act.at[k, core, 1, y_pos], y_across)):
                send(block, block, fwd_send.at[k], fwd_recv.at[k], my, peer)

    def forward(k):
        drain(act.at[k, core, 0], far_recv.at[k])

        @pl.when(k < straight)
        def _():
            for block in (act.at[k, core, 0, :, 1 - x_pos], act.at[k, core, 1, 1 - y_pos]):
                send(block, block, fwd_send.at[k], fwd_recv.at[k], my, partner)

    def contract(k):
        n = k // per_load
        step = lax.rem(k, per_load)

        @pl.when(step == 0)
        def _():
            load_down(n).wait()

        drain(act.at[k, 1 - core], fwd_recv.at[k])
        total = acc[...]
        for part in range(2):
            lhs = jnp.concatenate([act[k, part, way].reshape(rows, half // 2) for way in range(2)], axis=1)
            total = total + jnp.dot(lhs, wd_v[n, step, part], preferred_element_type=F32)
        acc[...] = total

    stages = tuple(zip((forward, gather, activate, combine, scatter, contract, multiply), lags))

    @pl.loop(0, chunks + max(lags))
    def _(t):
        for stage, lag in stages:
            @pl.when(jnp.logical_and(t >= lag, t < chunks + lag))
            def _():
                stage(t - lag)

    z_out[1] = acc[...].astype(BF16)
    z_copy = send(z_out.at[1], z_in.at[1], z_send.at[2], z_recv.at[2], 1 - my, mx)
    z_copy.wait()
    out_ref[...] = (m_v[...].astype(F32) + (z_out[1].astype(F32) + z_in[1].astype(F32))).astype(BF16)

    @pl.loop(0, chunks)
    def _(k):
        drain(theirs.at[k], pair_send.at[k])
        drain(hop_in.at[k], hop_send.at[k])
        drain(fin_in.at[k], fin_send.at[k])
        drain(act.at[k, core, 0, 0], near_send.at[k])
        drain(act.at[k, core, 0], far_send.at[k])
        drain(act.at[k, core], fwd_send.at[k])


def solution(mesh):
    mx_size = mesh.shape["mx"]
    act_spec = P(None, "mx")
    cache_spec = P("mx", None, "my", None)
    in_specs = (act_spec, P("mx"), P("mx"), P("mx"), P("mx", "my"), P("my"), P("mx", "my"), P("my"), P("mx", "my"), P("my"), P("my", "mx"), P("mx", "my"), P("mx", "my"), P("my", "mx"), cache_spec, cache_spec)
    out_specs = (act_spec, cache_spec, cache_spec)
    vmem = pl.BlockSpec(memory_space=pltpu.VMEM)
    anywhere = pl.BlockSpec(memory_space=pl.ANY)

    def local_layer(x_in, seq_lens, gain_attn, gain_mlp, w_q, b_q, w_k, b_k, w_v, b_v, w_o, w_gate, w_up, w_down, k_cache, v_cache):
        rows, cols = x_in.shape
        hidden = cols * mx_size
        q_cols = w_q.shape[1]
        kv_cols = w_k.shape[1]
        heads = q_cols // HEAD
        kv_heads = kv_cols // HEAD
        local_rows = rows // mx_size
        qkv_cols = q_cols + 2 * kv_cols
        first = 8 * HEAD
        rest = (q_cols - first) // 2
        pieces = ((0, 0, first, 0), (0, first, rest, first), (0, first + rest, rest, first + rest), (1, 0, kv_cols, q_cols), (2, 0, kv_cols, q_cols + kv_cols))
        inv_freq = ROPE_THETA ** (-2.0 * jnp.arange(HEAD // 2, dtype=F32) / HEAD)

        projected = pl.pallas_call(
            functools.partial(qkv_kernel, hidden, pieces),
            name="qkv",
            out_shape=jax.ShapeDtypeStruct((local_rows, qkv_cols), F32),
            in_specs=[vmem] + [anywhere] * 9,
            out_specs=vmem,
            scratch_shapes=[
                pltpu.SMEM((local_rows,), jnp.int32), VMEM((rows, cols), BF16), VMEM((cols,), BF16),
                VMEM(w_q.shape, BF16), VMEM(w_k.shape, BF16), VMEM(w_v.shape, BF16), VMEM(b_q.shape, BF16), VMEM(b_k.shape, BF16), VMEM(b_v.shape, BF16),
                VMEM((local_rows, HEAD), F32), VMEM((local_rows, HEAD), F32),
                VMEM((4, 2, local_rows, qkv_cols), BF16), VMEM((4, local_rows, qkv_cols), BF16), VMEM((3, local_rows, qkv_cols), BF16), VMEM((7, local_rows, first), BF16),
                VMEM((8, rows), F32), VMEM((8, 8, rows), F32),
                DMA((9,)), DMA((8,)), DMA((8,)), DMA((4,)), DMA((4,)), DMA((4, 3)), DMA((4, 3)), DMA((7,)), DMA((7,)),
            ],
            compiler_params=pltpu.CompilerParams(collective_id=0, has_side_effects=True, vmem_limit_bytes=16 * 2 ** 20),
            cost_estimate=pl.CostEstimate(flops=40_000_000_000, bytes_accessed=4_600_000, transcendentals=0),
        )(inv_freq, hbm(seq_lens), hbm(x_in), hbm(gain_attn), hbm(w_q), hbm(w_k), hbm(w_v), hbm(b_q), hbm(b_k), hbm(b_v))

        slots = k_cache.shape[1] * kv_heads
        flat = (local_rows, slots, HEAD)
        padded = (heads + 7) // 8 * 8
        k_flat, v_flat, attn = pl.pallas_call(
            functools.partial(attend_kernel, heads),
            name="attend",
            out_shape=(jax.ShapeDtypeStruct(flat, BF16), jax.ShapeDtypeStruct(flat, BF16), jax.ShapeDtypeStruct((local_rows, q_cols), BF16)),
            in_specs=[vmem] * 3 + [anywhere],
            out_specs=(anywhere, anywhere, vmem),
            scratch_shapes=[
                pltpu.SMEM((local_rows,), jnp.int32),
                VMEM((local_rows, padded, HEAD), F32), VMEM((local_rows, 16, HEAD), F32), VMEM((local_rows, 16, HEAD), F32), VMEM((local_rows, padded, HEAD), F32),
                VMEM((local_rows, 16, HEAD), BF16), VMEM((local_rows, 16, HEAD), BF16),
                DMA, DMA((2, local_rows)), DMA((2, local_rows)),
            ],
            compiler_params=pltpu.CompilerParams(vmem_limit_bytes=26 * 2 ** 20),
            cost_estimate=pl.CostEstimate(flops=20_000_000_000, bytes_accessed=17_000_000, transcendentals=0),
        )(projected, pltpu.with_memory_space_constraint(k_cache.reshape(flat), VMEM), pltpu.with_memory_space_constraint(v_cache.reshape(flat), VMEM), hbm(seq_lens))

        ff_cols = w_gate.shape[1]
        half = 768
        chunks = ff_cols // (2 * half)
        per_load = 1
        ring = 6
        loads = chunks // per_load
        lags = (17, 13, 9, 5, 2, 20, 0)
        x_out = pl.pallas_call(
            functools.partial(mlp_kernel, hidden, chunks, per_load, lags),
            name="mlp",
            out_shape=jax.ShapeDtypeStruct((rows, cols), BF16),
            in_specs=[vmem] + [anywhere] * 6,
            out_specs=vmem,
            scratch_shapes=[
                VMEM((rows, cols), BF16), VMEM((cols,), BF16),
                VMEM((8, local_rows, q_cols), BF16), VMEM(w_o.shape, BF16),
                VMEM((ring, cols, per_load * 2 * half), BF16), VMEM((ring, cols, per_load * 2 * half), BF16), VMEM((loads, per_load, 2, half, cols), BF16),
                VMEM((2, rows, cols), BF16), VMEM((2, rows, cols), BF16), VMEM((8, rows), F32), VMEM((8, 8, rows), F32),
                VMEM((rows, cols), BF16), VMEM((rows, cols), BF16), VMEM((rows, cols), F32),
            ] + [VMEM((chunks, 2, 2, 2, 2, 16, half // 2), BF16)] * 3 + [
                VMEM((chunks, 2, 2, 2, 16, half // 2), BF16), VMEM((chunks, 2, 2, 16, half // 2), BF16), VMEM((chunks, 2, 2, 2, 2, 16, half // 2), BF16),
                DMA((3,)), DMA((ring,)), DMA((ring,)), DMA((loads,)), DMA((8,)), DMA((8,)), DMA((3,)), DMA((3,)), DMA((8,)), DMA((8,)),
            ] + [DMA((chunks,))] * 12,
            compiler_params=pltpu.CompilerParams(collective_id=1, has_side_effects=True, vmem_limit_bytes=int(52.5 * 2 ** 20)),
            cost_estimate=pl.CostEstimate(flops=60_000_000_000, bytes_accessed=57_000_000, transcendentals=0),
        )(attn, hbm(x_in), hbm(gain_mlp), hbm(w_o), hbm(w_gate), hbm(w_up), hbm(w_down.reshape(loads, per_load, 2, half, cols)))
        return x_out, k_flat.reshape(k_cache.shape), v_flat.reshape(v_cache.shape)

    return jax.shard_map(local_layer, mesh=mesh, in_specs=in_specs, out_specs=out_specs, check_vma=False)
```

```python
import functools

import jax
import jax.numpy as jnp
from jax import lax
from jax.experimental import pallas as pl
from jax.experimental.pallas import tpu as pltpu
from jax.sharding import PartitionSpec as P

HEAD = 128
NORM_EPS = 1e-6
ROPE_THETA = 1000000.0
MESH = pl.DeviceIdType.MESH
F32 = jnp.float32
BF16 = jnp.bfloat16
VMEM = pltpu.VMEM
DMA = pltpu.SemaphoreType.DMA


def neighbours(mx):
    core = lax.rem(mx, 2)
    chip = mx // 2
    x_pos = lax.rem(chip, 2)
    y_pos = chip // 2
    others = (y_pos * 2 + (1 - x_pos), (1 - y_pos) * 2 + x_pos, (1 - y_pos) * 2 + (1 - x_pos))
    return core, chip, chip * 2 + (1 - core), others


def far_first(mx):
    core, chip, partner, others = neighbours(mx)
    return [other * 2 + c for other in (others[2], others[0], others[1]) for c in (core, 1 - core)] + [partner]


def hbm(array):
    return pltpu.with_memory_space_constraint(array, pltpu.HBM)


def send(src, dst, send_sem, recv_sem, my, mx):
    copy = pltpu.make_async_remote_copy(src_ref=src, dst_ref=dst, send_sem=send_sem, recv_sem=recv_sem, device_id=(my, mx), device_id_type=MESH)
    copy.start()
    return copy


def drain(ref, sem):
    pltpu.make_async_copy(ref, ref, sem).wait()


def share_stat(square_sum, my, mx, stat_out, stat_in, send_sems, recv_sems, between=None):
    rows = square_sum.shape[0]
    turned = jnp.transpose(jnp.broadcast_to(square_sum, (rows, 128)))[0:8]
    stat_out[...] = turned
    copies = []
    for step, peer in enumerate(far_first(mx)):
        copies.append(send(stat_out, stat_in.at[mx], send_sems.at[step], recv_sems.at[step], my, peer))
    stat_in[mx] = turned
    if between is not None:
        between()
    for copy in copies:
        copy.wait()
    total = jnp.sum(stat_in[...], axis=0)
    return jnp.transpose(jnp.broadcast_to(total[0:1], (128, rows)))[:, 0:1]


def enter(my, mx, with_z, meanwhile=None):
    barrier = pltpu.get_barrier_semaphore()
    for step in range(1, 8):
        pl.semaphore_signal(barrier, inc=1, device_id=(my, lax.rem(mx + step, 8)), device_id_type=MESH)
    if with_z:
        pl.semaphore_signal(barrier, inc=1, device_id=(1 - my, mx), device_id_type=MESH)
    if meanwhile is not None:
        meanwhile()
    pl.semaphore_wait(barrier, 8 if with_z else 7)


def qkv_kernel(hidden, pieces, freq_ref, lens_hbm, x_hbm, gain_hbm, wq_hbm, wk_hbm, wv_hbm, bq_hbm, bk_hbm, bv_hbm, out_ref,
               lens_s, x_v, gain_v, wq_v, wk_v, wv_v, bq_v, bk_v, bv_v, cos_v, sin_v, part, pair_in, chip_in, direct_in, stat_out, stat_in,
               w_sems, stat_send, stat_recv, pair_send, pair_recv, chip_send, chip_recv, direct_send, direct_recv):
    my = lax.axis_index("my")
    mx = lax.axis_index("mx")
    core, chip, partner, others = neighbours(mx)
    loads = [pltpu.make_async_copy(src, dst, w_sems.at[n]) for n, (src, dst) in enumerate((
        (wq_hbm, wq_v), (wk_hbm, wk_v), (wv_hbm, wv_v), (x_hbm, x_v), (gain_hbm, gain_v), (lens_hbm, lens_s), (bq_hbm, bq_v), (bk_hbm, bk_v), (bv_hbm, bv_v)))]
    loads[3].start()

    def meanwhile():
        for n in (4, 5, 0, 1, 2, 6, 7, 8):
            loads[n].start()
        loads[3].wait()

    enter(my, mx, False, meanwhile)
    x = x_v[...].astype(F32)
    square_sum = jnp.sum(x * x, axis=1, keepdims=True)

    def tables():
        loads[4].wait()
        loads[5].wait()
        rows = lens_s.shape[0]
        sub = lax.broadcasted_iota(jnp.int32, (rows, HEAD // 2), 0)
        position = jnp.zeros((rows, HEAD // 2), F32)
        for b in range(rows):
            position = jnp.where(sub == b, lens_s[b].astype(F32), position)
        angles = position * freq_ref[...][None, :]
        cos_half = jnp.cos(angles)
        sin_half = jnp.sin(angles)
        cos_v[...] = jnp.concatenate([cos_half, cos_half], axis=1)
        sin_v[...] = jnp.concatenate([-sin_half, sin_half], axis=1)
        for n in (0, 1, 2, 6, 7, 8):
            loads[n].wait()

    stat = share_stat(square_sum, my, mx, stat_out, stat_in, stat_send, stat_recv, tables)
    normed = (x * lax.rsqrt(stat / hidden + NORM_EPS) * gain_v[...].astype(F32)[None, :]).astype(BF16)
    weights = (wq_v, wk_v, wv_v)
    biases = (bq_v, bk_v, bv_v)
    copies = []
    pair_copies = []
    direct = []
    for n, (which, first, width, out_first) in enumerate(pieces):
        cols = pl.ds(out_first, width)
        product = jnp.dot(normed, weights[which][:, first:first + width], preferred_element_type=F32)
        part[:, :, :, cols] = product.reshape(4, 2, 8, width).astype(BF16)
        if n == 0:
            for k, peer in enumerate(far_first(mx)):
                direct.append(send(part.at[peer // 2, lax.rem(peer, 2), :, cols], direct_in.at[k], direct_send.at[k], direct_recv.at[k], my, peer))
        else:
            pair_copies.append(send(part.at[:, 1 - core, :, cols], pair_in.at[:, :, cols], pair_send.at[n - 1], pair_recv.at[n - 1], my, partner))
    for n, (which, first, width, out_first) in enumerate(pieces[1:]):
        cols = pl.ds(out_first, width)
        pair_copies[n].wait_recv()
        pair_in[:, :, cols] = (part[:, core, :, cols].astype(F32) + pair_in[:, :, cols].astype(F32)).astype(BF16)
        for k, other in enumerate(others):
            copies.append(send(pair_in.at[other, :, cols], chip_in.at[k, :, cols], chip_send.at[n, k], chip_recv.at[n, k], my, other * 2 + core))
    for n, (which, first, width, out_first) in enumerate(pieces):
        cols = pl.ds(out_first, width)
        if n == 0:
            total = part[chip, core, :, cols].astype(F32)
            for k in range(7):
                direct[k].wait_recv()
                total = total + direct_in[k].astype(F32)
        else:
            total = pair_in[chip, :, cols].astype(F32)
            for k in range(3):
                copies[(n - 1) * 3 + k].wait_recv()
                total = total + chip_in[k, :, cols].astype(F32)
        total = total + biases[which][first:first + width].astype(F32)[None, :]
        for h in range(0, width, HEAD):
            vals = total[:, h:h + HEAD]
            if which < 2:
                vals = vals * cos_v[...] + pltpu.roll(vals, HEAD // 2, 1) * sin_v[...]
            out_ref[:, out_first + h:out_first + h + HEAD] = vals
    for copy in direct + pair_copies + copies:
        copy.wait_send()


def attend_kernel(heads, proj_ref, k_ref, v_ref, lens_hbm, ko_hbm, vo_hbm, attn_ref,
                  lens_s, q_s, k_s, v_s, o_s, k_win, v_win, lens_sem, out_sems, win_sems):
    rows, slots, _ = k_ref.shape
    q_cols = heads * HEAD
    kv_cols = (proj_ref.shape[1] - q_cols) // 2
    kv_heads = kv_cols // HEAD
    group = heads // kv_heads
    load_lens = pltpu.make_async_copy(lens_hbm, lens_s, lens_sem)
    load_lens.start()
    outs = []
    for b in range(rows):
        outs.append((pltpu.make_async_copy(k_ref.at[b], ko_hbm.at[b], out_sems.at[0, b]), pltpu.make_async_copy(v_ref.at[b], vo_hbm.at[b], out_sems.at[1, b])))
        for out in outs[b]:
            out.start()
    q_s[...] = jnp.zeros_like(q_s)
    for h in range(heads):
        q_s[:, h, :] = proj_ref[:, h * HEAD:(h + 1) * HEAD]
    for h in range(kv_heads):
        k_new = proj_ref[:, q_cols + h * HEAD:q_cols + (h + 1) * HEAD]
        v_new = proj_ref[:, q_cols + kv_cols + h * HEAD:q_cols + kv_cols + (h + 1) * HEAD]
        for r in range(16 // kv_heads):
            k_s[:, r * kv_heads + h, :] = k_new
            v_s[:, r * kv_heads + h, :] = v_new
    load_lens.wait()
    q_pad = q_s.shape[1]
    per_tile = 16 // kv_heads
    sub = lax.broadcasted_iota(jnp.int32, (16, HEAD), 0) // kv_heads
    row = lax.broadcasted_iota(jnp.int32, (q_pad, 1), 0)
    row_head = sum((row >= group * n).astype(jnp.int32) for n in range(1, kv_heads))
    col = lax.broadcasted_iota(jnp.int32, (q_pad, slots), 1)
    offset = jnp.where(lax.rem(col, kv_heads) == row_head, col // kv_heads, slots)
    new_col = lax.broadcasted_iota(jnp.int32, (q_pad, 16), 1)

    def window(b, position):
        base = pl.multiple_of(position // per_tile * 16, 16)
        at_slot = sub == lax.rem(position, per_tile)
        for src, new, win in ((k_ref, k_s, k_win), (v_ref, v_s, v_win)):
            win[b] = jnp.where(at_slot, new[b], src[b, pl.ds(base, 16), :].astype(F32)).astype(BF16)

    def one_row(b):
        position = lens_s[b]
        if b < rows - 1:
            window(b, position)
        query = q_s[b].astype(BF16)
        scores = lax.dot_general(query, k_ref[b], (((1,), (1,)), ((), ())), preferred_element_type=F32) * HEAD ** -0.5
        scores = jnp.where(offset < position, scores, -jnp.inf)
        new_scores = lax.dot_general(query, k_s[b].astype(BF16), (((1,), (1,)), ((), ())), preferred_element_type=F32) * HEAD ** -0.5
        new_scores = jnp.where(new_col == row_head, new_scores, -jnp.inf)
        top = jnp.maximum(jnp.max(scores, axis=1, keepdims=True), jnp.max(new_scores, axis=1, keepdims=True))
        weights = jnp.exp(scores - top)
        new_weights = jnp.exp(new_scores - top)
        weight_sum = jnp.sum(weights, axis=1, keepdims=True) + jnp.sum(new_weights, axis=1, keepdims=True)
        weighted = jnp.dot(weights.astype(BF16), v_ref[b], preferred_element_type=F32)
        weighted = weighted + jnp.dot(new_weights.astype(BF16), v_s[b].astype(BF16), preferred_element_type=F32)
        o_s[b] = weighted / weight_sum

    def fix(b):
        base = pl.multiple_of(lens_s[b] // per_tile * 16, 16)
        return [pltpu.make_async_copy(win.at[b], hbm_out.at[b, pl.ds(base, 16), :], win_sems.at[n, b]) for n, (win, hbm_out) in enumerate(((k_win, ko_hbm), (v_win, vo_hbm)))]

    for b in range(rows - 1):
        one_row(b)
    window(rows - 1, lens_s[rows - 1])
    for b in range(rows):
        for out, win in zip(outs[b], fix(b)):
            out.wait()
            win.start()
    one_row(rows - 1)
    for h in range(heads):
        attn_ref[:, h * HEAD:(h + 1) * HEAD] = o_s[:, h, :].astype(BF16)
    for b in range(rows):
        for win in fix(b):
            win.wait()


def mlp_kernel(hidden, chunks, per_load, lags, attn_ref, x_hbm, gain_hbm, wo_hbm, wg_hbm, wu_hbm, wd_hbm, out_ref,
               x_v, gain_v, attn_all, wo_v, wg_v, wu_v, wd_v, z_out, z_in, stat_out, stat_in, h_v, m_v, acc, mine, theirs, pair_in, hop_in, fin_in, act,
               in_sems, wg_sems, wu_sems, wd_sems, ag_send, ag_recv, z_send, z_recv, stat_send, stat_recv,
               pair_send, pair_recv, hop_send, hop_recv, fin_send, fin_recv, near_send, near_recv, far_send, far_recv, fwd_send, fwd_recv):
    my = lax.axis_index("my")
    mx = lax.axis_index("mx")
    core, chip, partner, others = neighbours(mx)
    x_pos = lax.rem(chip, 2)
    y_pos = chip // 2
    x_peer = others[0] * 2 + core
    y_peer = others[1] * 2 + core
    x_across = others[0] * 2 + (1 - core)
    y_across = others[1] * 2 + (1 - core)
    straight = chunks - 1
    half = 2 * act.shape[6]
    loads = chunks // per_load
    load_cols = per_load * 2 * half
    ring = wg_v.shape[0]

    def load_gate(n):
        cols = pl.ds(pl.multiple_of(n * load_cols, 128), load_cols)
        slot = lax.rem(n, ring)
        return pltpu.make_async_copy(wg_hbm.at[:, cols], wg_v.at[slot], wg_sems.at[slot]), pltpu.make_async_copy(wu_hbm.at[:, cols], wu_v.at[slot], wu_sems.at[slot])

    def load_down(n):
        return pltpu.make_async_copy(wd_hbm.at[n], wd_v.at[n], wd_sems.at[n])

    firsts = [pltpu.make_async_copy(src, dst, in_sems.at[n]) for n, (src, dst) in enumerate(((wo_hbm, wo_v), (x_hbm, x_v), (gain_hbm, gain_v)))]

    def meanwhile():
        for first in firsts:
            first.start()

        @pl.loop(0, ring)
        def _(n):
            for load in load_gate(n):
                load.start()

        @pl.loop(0, loads)
        def _(n):
            load_down(n).start()

        attn_all[mx] = attn_ref[...]
        acc[...] = jnp.zeros_like(acc)

    enter(my, mx, True, meanwhile)

    copies = []
    for step, peer in enumerate(far_first(mx)):
        copies.append(send(attn_ref, attn_all.at[mx], ag_send.at[step], ag_recv.at[step], my, peer))
    for first in firsts:
        first.wait()
    for copy in copies:
        copy.wait()
    rows = x_v.shape[0]
    attn = attn_all[...].reshape(rows, attn_ref.shape[1])
    z_parts = (pl.ds(0, 384), pl.ds(384, x_v.shape[1] - 384))
    z_copies = []
    for n, part in enumerate(z_parts):
        z_out[0, :, part] = jnp.dot(attn, wo_v[:, part], preferred_element_type=F32).astype(BF16)
        z_copies.append(send(z_out.at[0, :, part], z_in.at[0, :, part], z_send.at[n], z_recv.at[n], 1 - my, mx))
    for z_copy in z_copies:
        z_copy.wait()
    mid = (x_v[...].astype(F32) + (z_out[0].astype(F32) + z_in[0].astype(F32))).astype(BF16)
    m_v[...] = mid
    mid = mid.astype(F32)
    stat = share_stat(jnp.sum(mid * mid, axis=1, keepdims=True), my, mx, stat_out, stat_in, stat_send, stat_recv)
    h_v[...] = (mid * lax.rsqrt(stat / hidden + NORM_EPS) * gain_v[...].astype(F32)[None, :]).astype(BF16)

    def multiply(k):
        n = k // per_load
        slot = lax.rem(n, ring)
        step = lax.rem(k, per_load)

        @pl.when(step == 0)
        def _():
            for load in load_gate(n):
                load.wait()

        h = h_v[...]

        def products(part, dest):
            cols = pl.ds(pl.multiple_of(step * (2 * half) + part * half, 128), half)
            for which, weights in ((0, wg_v), (1, wu_v)):
                out = jnp.dot(h, weights[slot, :, cols], preferred_element_type=F32).astype(BF16)
                for way in range(2):
                    dest[k, way, :, :, which] = out[:, way * half // 2:(way + 1) * half // 2].reshape(2, 2, 16, half // 2)

        products(1 - core, theirs)
        send(theirs.at[k], pair_in.at[k], pair_send.at[k], pair_recv.at[k], my, partner)
        products(core, mine)

        @pl.when(jnp.logical_and(step == per_load - 1, n + ring < loads))
        def _():
            for load in load_gate(n + ring):
                load.start()

    def scatter(k):
        drain(pair_in.at[k], pair_recv.at[k])
        pair_in[k] = (mine[k].astype(F32) + pair_in[k].astype(F32)).astype(BF16)
        send(pair_in.at[k, 0, :, 1 - x_pos], hop_in.at[k, 0], hop_send.at[k], hop_recv.at[k], my, x_peer)
        send(pair_in.at[k, 1, 1 - y_pos], hop_in.at[k, 1], hop_send.at[k], hop_recv.at[k], my, y_peer)

    def combine(k):
        drain(hop_in.at[k], hop_recv.at[k])
        hop_in[k, 0] = (pair_in[k, 0, :, x_pos].astype(F32) + hop_in[k, 0].astype(F32)).astype(BF16)
        hop_in[k, 1] = (pair_in[k, 1, y_pos].astype(F32) + hop_in[k, 1].astype(F32)).astype(BF16)
        send(hop_in.at[k, 0, 1 - y_pos], fin_in.at[k, 0], fin_send.at[k], fin_recv.at[k], my, y_peer)
        send(hop_in.at[k, 1, 1 - x_pos], fin_in.at[k, 1], fin_send.at[k], fin_recv.at[k], my, x_peer)

    def activate(k):
        drain(fin_in.at[k], fin_recv.at[k])
        for way, own in ((0, y_pos), (1, x_pos)):
            total = hop_in[k, way, own].astype(F32) + fin_in[k, way].astype(F32)
            gate = total[0]
            act[k, core, way, y_pos, x_pos] = (gate * jax.nn.sigmoid(gate) * total[1]).astype(BF16)
        for way, peer in ((0, y_peer), (1, x_peer)):
            block = act.at[k, core, way, y_pos, x_pos]
            send(block, block, near_send.at[k], near_recv.at[k], my, peer)
        both = act.at[k, core, :, y_pos, x_pos]
        send(both, both, fwd_send.at[k], fwd_recv.at[k], my, partner)

    def gather(k):
        drain(act.at[k, core, 0, 0], near_recv.at[k])
        for block, peer in ((act.at[k, core, 0, :, x_pos], x_peer), (act.at[k, core, 1, y_pos], y_peer)):
            send(block, block, far_send.at[k], far_recv.at[k], my, peer)
        for block in (act.at[k, core, 0, 1 - y_pos, x_pos], act.at[k, core, 1, y_pos, 1 - x_pos]):
            send(block, block, fwd_send.at[k], fwd_recv.at[k], my, partner)

        @pl.when(k >= straight)
        def _():
            for block, peer in ((act.at[k, core, 0, :, x_pos], x_across), (act.at[k, core, 1, y_pos], y_across)):
                send(block, block, fwd_send.at[k], fwd_recv.at[k], my, peer)

    def forward(k):
        drain(act.at[k, core, 0], far_recv.at[k])

        @pl.when(k < straight)
        def _():
            for block in (act.at[k, core, 0, :, 1 - x_pos], act.at[k, core, 1, 1 - y_pos]):
                send(block, block, fwd_send.at[k], fwd_recv.at[k], my, partner)

    def contract(k):
        n = k // per_load
        step = lax.rem(k, per_load)

        @pl.when(step == 0)
        def _():
            load_down(n).wait()

        drain(act.at[k, 1 - core], fwd_recv.at[k])
        total = acc[...]
        for part in range(2):
            lhs = jnp.concatenate([act[k, part, way].reshape(rows, half // 2) for way in range(2)], axis=1)
            total = total + jnp.dot(lhs, wd_v[n, step, part], preferred_element_type=F32)
        acc[...] = total

    stages = tuple(zip((forward, gather, activate, combine, scatter, contract, multiply), lags))

    @pl.loop(0, chunks + max(lags))
    def _(t):
        for stage, lag in stages:
            @pl.when(jnp.logical_and(t >= lag, t < chunks + lag))
            def _():
                stage(t - lag)

    z_out[1] = acc[...].astype(BF16)
    z_copy = send(z_out.at[1], z_in.at[1], z_send.at[2], z_recv.at[2], 1 - my, mx)
    z_copy.wait()
    out_ref[...] = (m_v[...].astype(F32) + (z_out[1].astype(F32) + z_in[1].astype(F32))).astype(BF16)

    @pl.loop(0, chunks)
    def _(k):
        drain(theirs.at[k], pair_send.at[k])
        drain(hop_in.at[k], hop_send.at[k])
        drain(fin_in.at[k], fin_send.at[k])
        drain(act.at[k, core, 0, 0], near_send.at[k])
        drain(act.at[k, core, 0], far_send.at[k])
        drain(act.at[k, core], fwd_send.at[k])


def solution(mesh):
    mx_size = mesh.shape["mx"]
    act_spec = P(None, "mx")
    cache_spec = P("mx", None, "my", None)
    in_specs = (act_spec, P("mx"), P("mx"), P("mx"), P("mx", "my"), P("my"), P("mx", "my"), P("my"), P("mx", "my"), P("my"), P("my", "mx"), P("mx", "my"), P("mx", "my"), P("my", "mx"), cache_spec, cache_spec)
    out_specs = (act_spec, cache_spec, cache_spec)
    vmem = pl.BlockSpec(memory_space=pltpu.VMEM)
    anywhere = pl.BlockSpec(memory_space=pl.ANY)

    def local_layer(x_in, seq_lens, gain_attn, gain_mlp, w_q, b_q, w_k, b_k, w_v, b_v, w_o, w_gate, w_up, w_down, k_cache, v_cache):
        rows, cols = x_in.shape
        hidden = cols * mx_size
        q_cols = w_q.shape[1]
        kv_cols = w_k.shape[1]
        heads = q_cols // HEAD
        kv_heads = kv_cols // HEAD
        local_rows = rows // mx_size
        qkv_cols = q_cols + 2 * kv_cols
        first = 8 * HEAD
        rest = (q_cols - first) // 2
        pieces = ((0, 0, first, 0), (0, first, rest, first), (0, first + rest, rest, first + rest), (1, 0, kv_cols, q_cols), (2, 0, kv_cols, q_cols + kv_cols))
        inv_freq = ROPE_THETA ** (-2.0 * jnp.arange(HEAD // 2, dtype=F32) / HEAD)

        projected = pl.pallas_call(
            functools.partial(qkv_kernel, hidden, pieces),
            name="qkv",
            out_shape=jax.ShapeDtypeStruct((local_rows, qkv_cols), F32),
            in_specs=[vmem] + [anywhere] * 9,
            out_specs=vmem,
            scratch_shapes=[
                pltpu.SMEM((local_rows,), jnp.int32), VMEM((rows, cols), BF16), VMEM((cols,), BF16),
                VMEM(w_q.shape, BF16), VMEM(w_k.shape, BF16), VMEM(w_v.shape, BF16), VMEM(b_q.shape, BF16), VMEM(b_k.shape, BF16), VMEM(b_v.shape, BF16),
                VMEM((local_rows, HEAD), F32), VMEM((local_rows, HEAD), F32),
                VMEM((4, 2, local_rows, qkv_cols), BF16), VMEM((4, local_rows, qkv_cols), BF16), VMEM((3, local_rows, qkv_cols), BF16), VMEM((7, local_rows, first), BF16),
                VMEM((8, rows), F32), VMEM((8, 8, rows), F32),
                DMA((9,)), DMA((8,)), DMA((8,)), DMA((4,)), DMA((4,)), DMA((4, 3)), DMA((4, 3)), DMA((7,)), DMA((7,)),
            ],
            compiler_params=pltpu.CompilerParams(collective_id=0, has_side_effects=True, vmem_limit_bytes=16 * 2 ** 20),
            cost_estimate=pl.CostEstimate(flops=40_000_000_000, bytes_accessed=4_600_000, transcendentals=0),
        )(inv_freq, hbm(seq_lens), hbm(x_in), hbm(gain_attn), hbm(w_q), hbm(w_k), hbm(w_v), hbm(b_q), hbm(b_k), hbm(b_v))

        slots = k_cache.shape[1] * kv_heads
        flat = (local_rows, slots, HEAD)
        padded = (heads + 7) // 8 * 8
        k_flat, v_flat, attn = pl.pallas_call(
            functools.partial(attend_kernel, heads),
            name="attend",
            out_shape=(jax.ShapeDtypeStruct(flat, BF16), jax.ShapeDtypeStruct(flat, BF16), jax.ShapeDtypeStruct((local_rows, q_cols), BF16)),
            in_specs=[vmem] * 3 + [anywhere],
            out_specs=(anywhere, anywhere, vmem),
            scratch_shapes=[
                pltpu.SMEM((local_rows,), jnp.int32),
                VMEM((local_rows, padded, HEAD), F32), VMEM((local_rows, 16, HEAD), F32), VMEM((local_rows, 16, HEAD), F32), VMEM((local_rows, padded, HEAD), F32),
                VMEM((local_rows, 16, HEAD), BF16), VMEM((local_rows, 16, HEAD), BF16),
                DMA, DMA((2, local_rows)), DMA((2, local_rows)),
            ],
            compiler_params=pltpu.CompilerParams(vmem_limit_bytes=26 * 2 ** 20),
            cost_estimate=pl.CostEstimate(flops=20_000_000_000, bytes_accessed=17_000_000, transcendentals=0),
        )(projected, pltpu.with_memory_space_constraint(k_cache.reshape(flat), VMEM), pltpu.with_memory_space_constraint(v_cache.reshape(flat), VMEM), hbm(seq_lens))

        ff_cols = w_gate.shape[1]
        half = 768
        chunks = ff_cols // (2 * half)
        per_load = 1
        ring = 6
        loads = chunks // per_load
        lags = (21, 16, 11, 7, 2, 24, 0)
        x_out = pl.pallas_call(
            functools.partial(mlp_kernel, hidden, chunks, per_load, lags),
            name="mlp",
            out_shape=jax.ShapeDtypeStruct((rows, cols), BF16),
            in_specs=[vmem] + [anywhere] * 6,
            out_specs=vmem,
            scratch_shapes=[
                VMEM((rows, cols), BF16), VMEM((cols,), BF16),
                VMEM((8, local_rows, q_cols), BF16), VMEM(w_o.shape, BF16),
                VMEM((ring, cols, per_load * 2 * half), BF16), VMEM((ring, cols, per_load * 2 * half), BF16), VMEM((loads, per_load, 2, half, cols), BF16),
                VMEM((2, rows, cols), BF16), VMEM((2, rows, cols), BF16), VMEM((8, rows), F32), VMEM((8, 8, rows), F32),
                VMEM((rows, cols), BF16), VMEM((rows, cols), BF16), VMEM((rows, cols), F32),
            ] + [VMEM((chunks, 2, 2, 2, 2, 16, half // 2), BF16)] * 3 + [
                VMEM((chunks, 2, 2, 2, 16, half // 2), BF16), VMEM((chunks, 2, 2, 16, half // 2), BF16), VMEM((chunks, 2, 2, 2, 2, 16, half // 2), BF16),
                DMA((3,)), DMA((ring,)), DMA((ring,)), DMA((loads,)), DMA((8,)), DMA((8,)), DMA((3,)), DMA((3,)), DMA((8,)), DMA((8,)),
            ] + [DMA((chunks,))] * 12,
            compiler_params=pltpu.CompilerParams(collective_id=1, has_side_effects=True, vmem_limit_bytes=int(52.5 * 2 ** 20)),
            cost_estimate=pl.CostEstimate(flops=60_000_000_000, bytes_accessed=57_000_000, transcendentals=0),
        )(attn, hbm(x_in), hbm(gain_mlp), hbm(w_o), hbm(w_gate), hbm(w_up), hbm(w_down.reshape(loads, per_load, 2, half, cols)))
        return x_out, k_flat.reshape(k_cache.shape), v_flat.reshape(v_cache.shape)

    return jax.shard_map(local_layer, mesh=mesh, in_specs=in_specs, out_specs=out_specs, check_vma=False)
```

```python
import functools

import jax
import jax.numpy as jnp
from jax import lax
from jax.experimental import pallas as pl
from jax.experimental.pallas import tpu as pltpu
from jax.sharding import PartitionSpec as P

HEAD = 128
NORM_EPS = 1e-6
ROPE_THETA = 1000000.0
MESH = pl.DeviceIdType.MESH
F32 = jnp.float32
BF16 = jnp.bfloat16
VMEM = pltpu.VMEM
DMA = pltpu.SemaphoreType.DMA


def neighbours(mx):
    core = lax.rem(mx, 2)
    chip = mx // 2
    x_pos = lax.rem(chip, 2)
    y_pos = chip // 2
    others = (y_pos * 2 + (1 - x_pos), (1 - y_pos) * 2 + x_pos, (1 - y_pos) * 2 + (1 - x_pos))
    return core, chip, chip * 2 + (1 - core), others


def far_first(mx):
    core, chip, partner, others = neighbours(mx)
    return [other * 2 + c for other in (others[2], others[0], others[1]) for c in (core, 1 - core)] + [partner]


def hbm(array):
    return pltpu.with_memory_space_constraint(array, pltpu.HBM)


def send(src, dst, send_sem, recv_sem, my, mx):
    copy = pltpu.make_async_remote_copy(src_ref=src, dst_ref=dst, send_sem=send_sem, recv_sem=recv_sem, device_id=(my, mx), device_id_type=MESH)
    copy.start()
    return copy


def drain(ref, sem):
    pltpu.make_async_copy(ref, ref, sem).wait()


def share_stat(square_sum, my, mx, stat_out, stat_in, send_sems, recv_sems, between=None):
    rows = square_sum.shape[0]
    turned = jnp.transpose(jnp.broadcast_to(square_sum, (rows, 128)))[0:8]
    stat_out[...] = turned
    copies = []
    for step, peer in enumerate(far_first(mx)):
        copies.append(send(stat_out, stat_in.at[mx], send_sems.at[step], recv_sems.at[step], my, peer))
    stat_in[mx] = turned
    if between is not None:
        between()
    for copy in copies:
        copy.wait()
    total = jnp.sum(stat_in[...], axis=0)
    return jnp.transpose(jnp.broadcast_to(total[0:1], (128, rows)))[:, 0:1]


def enter(my, mx, with_z, meanwhile=None):
    barrier = pltpu.get_barrier_semaphore()
    for step in range(1, 8):
        pl.semaphore_signal(barrier, inc=1, device_id=(my, lax.rem(mx + step, 8)), device_id_type=MESH)
    if with_z:
        pl.semaphore_signal(barrier, inc=1, device_id=(1 - my, mx), device_id_type=MESH)
    if meanwhile is not None:
        meanwhile()
    pl.semaphore_wait(barrier, 8 if with_z else 7)


def qkv_kernel(hidden, pieces, freq_ref, lens_hbm, x_hbm, gain_hbm, wq_hbm, wk_hbm, wv_hbm, bq_hbm, bk_hbm, bv_hbm, out_ref,
               lens_s, x_v, gain_v, wq_v, wk_v, wv_v, bq_v, bk_v, bv_v, cos_v, sin_v, part, pair_in, chip_in, direct_in, stat_out, stat_in,
               w_sems, stat_send, stat_recv, pair_send, pair_recv, chip_send, chip_recv, direct_send, direct_recv):
    my = lax.axis_index("my")
    mx = lax.axis_index("mx")
    core, chip, partner, others = neighbours(mx)
    loads = [pltpu.make_async_copy(src, dst, w_sems.at[n]) for n, (src, dst) in enumerate((
        (wq_hbm, wq_v), (wk_hbm, wk_v), (wv_hbm, wv_v), (x_hbm, x_v), (gain_hbm, gain_v), (lens_hbm, lens_s), (bq_hbm, bq_v), (bk_hbm, bk_v), (bv_hbm, bv_v)))]
    loads[3].start()

    def meanwhile():
        for n in (4, 5, 0, 1, 2, 6, 7, 8):
            loads[n].start()
        loads[3].wait()

    enter(my, mx, False, meanwhile)
    x = x_v[...].astype(F32)
    square_sum = jnp.sum(x * x, axis=1, keepdims=True)

    def tables():
        loads[4].wait()
        loads[5].wait()
        rows = lens_s.shape[0]
        sub = lax.broadcasted_iota(jnp.int32, (rows, HEAD // 2), 0)
        position = jnp.zeros((rows, HEAD // 2), F32)
        for b in range(rows):
            position = jnp.where(sub == b, lens_s[b].astype(F32), position)
        angles = position * freq_ref[...][None, :]
        cos_half = jnp.cos(angles)
        sin_half = jnp.sin(angles)
        cos_v[...] = jnp.concatenate([cos_half, cos_half], axis=1)
        sin_v[...] = jnp.concatenate([-sin_half, sin_half], axis=1)
        for n in (0, 1, 2, 6, 7, 8):
            loads[n].wait()

    stat = share_stat(square_sum, my, mx, stat_out, stat_in, stat_send, stat_recv, tables)
    normed = (x * lax.rsqrt(stat / hidden + NORM_EPS) * gain_v[...].astype(F32)[None, :]).astype(BF16)
    weights = (wq_v, wk_v, wv_v)
    biases = (bq_v, bk_v, bv_v)
    copies = []
    pair_copies = []
    direct = []
    for n, (which, first, width, out_first) in enumerate(pieces):
        cols = pl.ds(out_first, width)
        product = jnp.dot(normed, weights[which][:, first:first + width], preferred_element_type=F32)
        part[:, :, :, cols] = product.reshape(4, 2, 8, width).astype(BF16)
        if n == 0:
            for k, peer in enumerate(far_first(mx)):
                direct.append(send(part.at[peer // 2, lax.rem(peer, 2), :, cols], direct_in.at[k], direct_send.at[k], direct_recv.at[k], my, peer))
        else:
            pair_copies.append(send(part.at[:, 1 - core, :, cols], pair_in.at[:, :, cols], pair_send.at[n - 1], pair_recv.at[n - 1], my, partner))
    for n, (which, first, width, out_first) in enumerate(pieces[1:]):
        cols = pl.ds(out_first, width)
        pair_copies[n].wait_recv()
        pair_in[:, :, cols] = (part[:, core, :, cols].astype(F32) + pair_in[:, :, cols].astype(F32)).astype(BF16)
        for k, other in enumerate(others):
            copies.append(send(pair_in.at[other, :, cols], chip_in.at[k, :, cols], chip_send.at[n, k], chip_recv.at[n, k], my, other * 2 + core))
    for n, (which, first, width, out_first) in enumerate(pieces):
        cols = pl.ds(out_first, width)
        if n == 0:
            total = part[chip, core, :, cols].astype(F32)
            for k in range(7):
                direct[k].wait_recv()
                total = total + direct_in[k].astype(F32)
        else:
            total = pair_in[chip, :, cols].astype(F32)
            for k in range(3):
                copies[(n - 1) * 3 + k].wait_recv()
                total = total + chip_in[k, :, cols].astype(F32)
        total = total + biases[which][first:first + width].astype(F32)[None, :]
        for h in range(0, width, HEAD):
            vals = total[:, h:h + HEAD]
            if which < 2:
                vals = vals * cos_v[...] + pltpu.roll(vals, HEAD // 2, 1) * sin_v[...]
            out_ref[:, out_first + h:out_first + h + HEAD] = vals
    for copy in direct + pair_copies + copies:
        copy.wait_send()


def attend_kernel(heads, proj_ref, k_ref, v_ref, lens_hbm, ko_hbm, vo_hbm, attn_ref,
                  lens_s, q_s, k_s, v_s, o_s, k_win, v_win, lens_sem, out_sems, win_sems):
    rows, slots, _ = k_ref.shape
    q_cols = heads * HEAD
    kv_cols = (proj_ref.shape[1] - q_cols) // 2
    kv_heads = kv_cols // HEAD
    group = heads // kv_heads
    load_lens = pltpu.make_async_copy(lens_hbm, lens_s, lens_sem)
    load_lens.start()
    outs = []
    for b in range(rows):
        outs.append((pltpu.make_async_copy(k_ref.at[b], ko_hbm.at[b], out_sems.at[0, b]), pltpu.make_async_copy(v_ref.at[b], vo_hbm.at[b], out_sems.at[1, b])))
        for out in outs[b]:
            out.start()
    q_s[...] = jnp.zeros_like(q_s)
    for h in range(heads):
        q_s[:, h, :] = proj_ref[:, h * HEAD:(h + 1) * HEAD]
    for h in range(kv_heads):
        k_new = proj_ref[:, q_cols + h * HEAD:q_cols + (h + 1) * HEAD]
        v_new = proj_ref[:, q_cols + kv_cols + h * HEAD:q_cols + kv_cols + (h + 1) * HEAD]
        for r in range(16 // kv_heads):
            k_s[:, r * kv_heads + h, :] = k_new
            v_s[:, r * kv_heads + h, :] = v_new
    load_lens.wait()
    q_pad = q_s.shape[1]
    per_tile = 16 // kv_heads
    sub = lax.broadcasted_iota(jnp.int32, (16, HEAD), 0) // kv_heads
    row = lax.broadcasted_iota(jnp.int32, (q_pad, 1), 0)
    row_head = sum((row >= group * n).astype(jnp.int32) for n in range(1, kv_heads))
    col = lax.broadcasted_iota(jnp.int32, (q_pad, slots), 1)
    offset = jnp.where(lax.rem(col, kv_heads) == row_head, col // kv_heads, slots)
    new_col = lax.broadcasted_iota(jnp.int32, (q_pad, 16), 1)

    def window(b, position):
        base = pl.multiple_of(position // per_tile * 16, 16)
        at_slot = sub == lax.rem(position, per_tile)
        for src, new, win in ((k_ref, k_s, k_win), (v_ref, v_s, v_win)):
            win[b] = jnp.where(at_slot, new[b], src[b, pl.ds(base, 16), :].astype(F32)).astype(BF16)

    def one_row(b):
        position = lens_s[b]
        if b < rows - 1:
            window(b, position)
        query = q_s[b].astype(BF16)
        scores = lax.dot_general(query, k_ref[b], (((1,), (1,)), ((), ())), preferred_element_type=F32) * HEAD ** -0.5
        scores = jnp.where(offset < position, scores, -jnp.inf)
        new_scores = lax.dot_general(query, k_s[b].astype(BF16), (((1,), (1,)), ((), ())), preferred_element_type=F32) * HEAD ** -0.5
        new_scores = jnp.where(new_col == row_head, new_scores, -jnp.inf)
        top = jnp.maximum(jnp.max(scores, axis=1, keepdims=True), jnp.max(new_scores, axis=1, keepdims=True))
        weights = jnp.exp(scores - top)
        new_weights = jnp.exp(new_scores - top)
        weight_sum = jnp.sum(weights, axis=1, keepdims=True) + jnp.sum(new_weights, axis=1, keepdims=True)
        weighted = jnp.dot(weights.astype(BF16), v_ref[b], preferred_element_type=F32)
        weighted = weighted + jnp.dot(new_weights.astype(BF16), v_s[b].astype(BF16), preferred_element_type=F32)
        o_s[b] = weighted / weight_sum

    def fix(b):
        base = pl.multiple_of(lens_s[b] // per_tile * 16, 16)
        return [pltpu.make_async_copy(win.at[b], hbm_out.at[b, pl.ds(base, 16), :], win_sems.at[n, b]) for n, (win, hbm_out) in enumerate(((k_win, ko_hbm), (v_win, vo_hbm)))]

    for b in range(rows - 1):
        one_row(b)
    window(rows - 1, lens_s[rows - 1])
    for b in range(rows):
        for out, win in zip(outs[b], fix(b)):
            out.wait()
            win.start()
    one_row(rows - 1)
    for h in range(heads):
        attn_ref[:, h * HEAD:(h + 1) * HEAD] = o_s[:, h, :].astype(BF16)
    for b in range(rows):
        for win in fix(b):
            win.wait()


def mlp_kernel(hidden, chunks, per_load, lags, attn_ref, x_hbm, gain_hbm, wo_hbm, wg_hbm, wu_hbm, wd_hbm, out_ref,
               x_v, gain_v, attn_all, wo_v, wg_v, wu_v, wd_v, z_out, z_in, stat_out, stat_in, h_v, m_v, acc, mine, theirs, pair_in, hop_in, fin_in, act,
               in_sems, wg_sems, wu_sems, wd_sems, ag_send, ag_recv, z_send, z_recv, stat_send, stat_recv,
               pair_send, pair_recv, hop_send, hop_recv, fin_send, fin_recv, near_send, near_recv, far_send, far_recv, fwd_send, fwd_recv):
    my = lax.axis_index("my")
    mx = lax.axis_index("mx")
    core, chip, partner, others = neighbours(mx)
    x_pos = lax.rem(chip, 2)
    y_pos = chip // 2
    x_peer = others[0] * 2 + core
    y_peer = others[1] * 2 + core
    x_across = others[0] * 2 + (1 - core)
    y_across = others[1] * 2 + (1 - core)
    straight = chunks - 1
    half = 2 * act.shape[6]
    loads = chunks // per_load
    load_cols = per_load * 2 * half
    ring = wg_v.shape[0]

    def load_gate(n):
        cols = pl.ds(pl.multiple_of(n * load_cols, 128), load_cols)
        slot = lax.rem(n, ring)
        return pltpu.make_async_copy(wg_hbm.at[:, cols], wg_v.at[slot], wg_sems.at[slot]), pltpu.make_async_copy(wu_hbm.at[:, cols], wu_v.at[slot], wu_sems.at[slot])

    def load_down(n):
        return pltpu.make_async_copy(wd_hbm.at[n], wd_v.at[n], wd_sems.at[n])

    firsts = [pltpu.make_async_copy(src, dst, in_sems.at[n]) for n, (src, dst) in enumerate(((wo_hbm, wo_v), (x_hbm, x_v), (gain_hbm, gain_v)))]

    def meanwhile():
        for first in firsts:
            first.start()

        @pl.loop(0, ring)
        def _(n):
            for load in load_gate(n):
                load.start()

        @pl.loop(0, loads)
        def _(n):
            load_down(n).start()

        attn_all[mx] = attn_ref[...]
        acc[...] = jnp.zeros_like(acc)

    enter(my, mx, True, meanwhile)

    others = (others[2], others[0], others[1])
    shared = pl.ds(0, 12 * HEAD)
    direct = pl.ds(12 * HEAD, attn_ref.shape[1] - 12 * HEAD)
    spread = [send(attn_ref.at[:, shared], attn_all.at[mx, :, shared], ag_send.at[k], ag_recv.at[k], my, other * 2 + core) for k, other in enumerate(others)]
    passed = [send(attn_ref, attn_all.at[mx], ag_send.at[3], ag_recv.at[3], my, partner)]
    for k, other in enumerate(others):
        for n, peer in enumerate((other * 2 + core, other * 2 + (1 - core))):
            slot = 4 + 2 * k + n
            passed.append(send(attn_ref.at[:, direct], attn_all.at[mx, :, direct], ag_send.at[slot], ag_recv.at[slot], my, peer))
    for k, other in enumerate(others):
        spread[k].wait()
        block = attn_all.at[other * 2 + core, :, shared]
        passed.append(send(block, block, ag_send.at[10 + k], ag_recv.at[10 + k], my, partner))
    for first in firsts:
        first.wait()
    for copy in passed:
        copy.wait()
    rows = x_v.shape[0]
    attn = attn_all[...].reshape(rows, attn_ref.shape[1])
    z_parts = (pl.ds(0, 384), pl.ds(384, x_v.shape[1] - 384))
    z_copies = []
    for n, part in enumerate(z_parts):
        z_out[0, :, part] = jnp.dot(attn, wo_v[:, part], preferred_element_type=F32).astype(BF16)
        z_copies.append(send(z_out.at[0, :, part], z_in.at[0, :, part], z_send.at[n], z_recv.at[n], 1 - my, mx))
    for z_copy in z_copies:
        z_copy.wait()
    mid = (x_v[...].astype(F32) + (z_out[0].astype(F32) + z_in[0].astype(F32))).astype(BF16)
    m_v[...] = mid
    mid = mid.astype(F32)
    stat = share_stat(jnp.sum(mid * mid, axis=1, keepdims=True), my, mx, stat_out, stat_in, stat_send, stat_recv)
    h_v[...] = (mid * lax.rsqrt(stat / hidden + NORM_EPS) * gain_v[...].astype(F32)[None, :]).astype(BF16)

    def multiply(k):
        n = k // per_load
        slot = lax.rem(n, ring)
        step = lax.rem(k, per_load)

        @pl.when(step == 0)
        def _():
            for load in load_gate(n):
                load.wait()

        h = h_v[...]

        def products(part, dest):
            cols = pl.ds(pl.multiple_of(step * (2 * half) + part * half, 128), half)
            for which, weights in ((0, wg_v), (1, wu_v)):
                out = jnp.dot(h, weights[slot, :, cols], preferred_element_type=F32).astype(BF16)
                for way in range(2):
                    dest[k, way, :, :, which] = out[:, way * half // 2:(way + 1) * half // 2].reshape(2, 2, 16, half // 2)

        products(1 - core, theirs)
        send(theirs.at[k], pair_in.at[k], pair_send.at[k], pair_recv.at[k], my, partner)
        products(core, mine)

        @pl.when(jnp.logical_and(step == per_load - 1, n + ring < loads))
        def _():
            for load in load_gate(n + ring):
                load.start()

    def scatter(k):
        drain(pair_in.at[k], pair_recv.at[k])
        pair_in[k] = (mine[k].astype(F32) + pair_in[k].astype(F32)).astype(BF16)
        send(pair_in.at[k, 0, :, 1 - x_pos], hop_in.at[k, 0], hop_send.at[k], hop_recv.at[k], my, x_peer)
        send(pair_in.at[k, 1, 1 - y_pos], hop_in.at[k, 1], hop_send.at[k], hop_recv.at[k], my, y_peer)

    def combine(k):
        drain(hop_in.at[k], hop_recv.at[k])
        hop_in[k, 0] = (pair_in[k, 0, :, x_pos].astype(F32) + hop_in[k, 0].astype(F32)).astype(BF16)
        hop_in[k, 1] = (pair_in[k, 1, y_pos].astype(F32) + hop_in[k, 1].astype(F32)).astype(BF16)
        send(hop_in.at[k, 0, 1 - y_pos], fin_in.at[k, 0], fin_send.at[k], fin_recv.at[k], my, y_peer)
        send(hop_in.at[k, 1, 1 - x_pos], fin_in.at[k, 1], fin_send.at[k], fin_recv.at[k], my, x_peer)

    def activate(k):
        drain(fin_in.at[k], fin_recv.at[k])
        for way, own in ((0, y_pos), (1, x_pos)):
            total = hop_in[k, way, own].astype(F32) + fin_in[k, way].astype(F32)
            gate = total[0]
            act[k, core, way, y_pos, x_pos] = (gate * jax.nn.sigmoid(gate) * total[1]).astype(BF16)
        for way, peer in ((0, y_peer), (1, x_peer)):
            block = act.at[k, core, way, y_pos, x_pos]
            send(block, block, near_send.at[k], near_recv.at[k], my, peer)
        both = act.at[k, core, :, y_pos, x_pos]
        send(both, both, fwd_send.at[k], fwd_recv.at[k], my, partner)

    def gather(k):
        drain(act.at[k, core, 0, 0], near_recv.at[k])
        for block, peer in ((act.at[k, core, 0, :, x_pos], x_peer), (act.at[k, core, 1, y_pos], y_peer)):
            send(block, block, far_send.at[k], far_recv.at[k], my, peer)
        for block in (act.at[k, core, 0, 1 - y_pos, x_pos], act.at[k, core, 1, y_pos, 1 - x_pos]):
            send(block, block, fwd_send.at[k], fwd_recv.at[k], my, partner)

        @pl.when(k >= straight)
        def _():
            for block, peer in ((act.at[k, core, 0, :, x_pos], x_across), (act.at[k, core, 1, y_pos], y_across)):
                send(block, block, fwd_send.at[k], fwd_recv.at[k], my, peer)

    def forward(k):
        drain(act.at[k, core, 0], far_recv.at[k])

        @pl.when(k < straight)
        def _():
            for block in (act.at[k, core, 0, :, 1 - x_pos], act.at[k, core, 1, 1 - y_pos]):
                send(block, block, fwd_send.at[k], fwd_recv.at[k], my, partner)

    def contract(k):
        n = k // per_load
        step = lax.rem(k, per_load)

        @pl.when(step == 0)
        def _():
            load_down(n).wait()

        drain(act.at[k, 1 - core], fwd_recv.at[k])
        total = acc[...]
        for part in range(2):
            lhs = jnp.concatenate([act[k, part, way].reshape(rows, half // 2) for way in range(2)], axis=1)
            total = total + jnp.dot(lhs, wd_v[n, step, part], preferred_element_type=F32)
        acc[...] = total

    stages = tuple(zip((forward, gather, activate, combine, scatter, contract, multiply), lags))

    @pl.loop(0, chunks + max(lags))
    def _(t):
        for stage, lag in stages:
            @pl.when(jnp.logical_and(t >= lag, t < chunks + lag))
            def _():
                stage(t - lag)

    z_out[1] = acc[...].astype(BF16)
    z_copy = send(z_out.at[1], z_in.at[1], z_send.at[2], z_recv.at[2], 1 - my, mx)
    z_copy.wait()
    out_ref[...] = (m_v[...].astype(F32) + (z_out[1].astype(F32) + z_in[1].astype(F32))).astype(BF16)

    @pl.loop(0, chunks)
    def _(k):
        drain(theirs.at[k], pair_send.at[k])
        drain(hop_in.at[k], hop_send.at[k])
        drain(fin_in.at[k], fin_send.at[k])
        drain(act.at[k, core, 0, 0], near_send.at[k])
        drain(act.at[k, core, 0], far_send.at[k])
        drain(act.at[k, core], fwd_send.at[k])


def solution(mesh):
    mx_size = mesh.shape["mx"]
    act_spec = P(None, "mx")
    cache_spec = P("mx", None, "my", None)
    in_specs = (act_spec, P("mx"), P("mx"), P("mx"), P("mx", "my"), P("my"), P("mx", "my"), P("my"), P("mx", "my"), P("my"), P("my", "mx"), P("mx", "my"), P("mx", "my"), P("my", "mx"), cache_spec, cache_spec)
    out_specs = (act_spec, cache_spec, cache_spec)
    vmem = pl.BlockSpec(memory_space=pltpu.VMEM)
    anywhere = pl.BlockSpec(memory_space=pl.ANY)

    def local_layer(x_in, seq_lens, gain_attn, gain_mlp, w_q, b_q, w_k, b_k, w_v, b_v, w_o, w_gate, w_up, w_down, k_cache, v_cache):
        rows, cols = x_in.shape
        hidden = cols * mx_size
        q_cols = w_q.shape[1]
        kv_cols = w_k.shape[1]
        heads = q_cols // HEAD
        kv_heads = kv_cols // HEAD
        local_rows = rows // mx_size
        qkv_cols = q_cols + 2 * kv_cols
        first = 8 * HEAD
        rest = (q_cols - first) // 2
        pieces = ((0, 0, first, 0), (0, first, rest, first), (0, first + rest, rest, first + rest), (1, 0, kv_cols, q_cols), (2, 0, kv_cols, q_cols + kv_cols))
        inv_freq = ROPE_THETA ** (-2.0 * jnp.arange(HEAD // 2, dtype=F32) / HEAD)

        projected = pl.pallas_call(
            functools.partial(qkv_kernel, hidden, pieces),
            name="qkv",
            out_shape=jax.ShapeDtypeStruct((local_rows, qkv_cols), F32),
            in_specs=[vmem] + [anywhere] * 9,
            out_specs=vmem,
            scratch_shapes=[
                pltpu.SMEM((local_rows,), jnp.int32), VMEM((rows, cols), BF16), VMEM((cols,), BF16),
                VMEM(w_q.shape, BF16), VMEM(w_k.shape, BF16), VMEM(w_v.shape, BF16), VMEM(b_q.shape, BF16), VMEM(b_k.shape, BF16), VMEM(b_v.shape, BF16),
                VMEM((local_rows, HEAD), F32), VMEM((local_rows, HEAD), F32),
                VMEM((4, 2, local_rows, qkv_cols), BF16), VMEM((4, local_rows, qkv_cols), BF16), VMEM((3, local_rows, qkv_cols), BF16), VMEM((7, local_rows, first), BF16),
                VMEM((8, rows), F32), VMEM((8, 8, rows), F32),
                DMA((9,)), DMA((8,)), DMA((8,)), DMA((4,)), DMA((4,)), DMA((4, 3)), DMA((4, 3)), DMA((7,)), DMA((7,)),
            ],
            compiler_params=pltpu.CompilerParams(collective_id=0, has_side_effects=True, vmem_limit_bytes=16 * 2 ** 20),
            cost_estimate=pl.CostEstimate(flops=40_000_000_000, bytes_accessed=4_600_000, transcendentals=0),
        )(inv_freq, hbm(seq_lens), hbm(x_in), hbm(gain_attn), hbm(w_q), hbm(w_k), hbm(w_v), hbm(b_q), hbm(b_k), hbm(b_v))

        slots = k_cache.shape[1] * kv_heads
        flat = (local_rows, slots, HEAD)
        padded = (heads + 7) // 8 * 8
        k_flat, v_flat, attn = pl.pallas_call(
            functools.partial(attend_kernel, heads),
            name="attend",
            out_shape=(jax.ShapeDtypeStruct(flat, BF16), jax.ShapeDtypeStruct(flat, BF16), jax.ShapeDtypeStruct((local_rows, q_cols), BF16)),
            in_specs=[vmem] * 3 + [anywhere],
            out_specs=(anywhere, anywhere, vmem),
            scratch_shapes=[
                pltpu.SMEM((local_rows,), jnp.int32),
                VMEM((local_rows, padded, HEAD), F32), VMEM((local_rows, 16, HEAD), F32), VMEM((local_rows, 16, HEAD), F32), VMEM((local_rows, padded, HEAD), F32),
                VMEM((local_rows, 16, HEAD), BF16), VMEM((local_rows, 16, HEAD), BF16),
                DMA, DMA((2, local_rows)), DMA((2, local_rows)),
            ],
            compiler_params=pltpu.CompilerParams(vmem_limit_bytes=26 * 2 ** 20),
            cost_estimate=pl.CostEstimate(flops=20_000_000_000, bytes_accessed=17_000_000, transcendentals=0),
        )(projected, pltpu.with_memory_space_constraint(k_cache.reshape(flat), VMEM), pltpu.with_memory_space_constraint(v_cache.reshape(flat), VMEM), hbm(seq_lens))

        ff_cols = w_gate.shape[1]
        half = 768
        chunks = ff_cols // (2 * half)
        per_load = 1
        ring = 6
        loads = chunks // per_load
        lags = (21, 16, 11, 7, 2, 24, 0)
        x_out = pl.pallas_call(
            functools.partial(mlp_kernel, hidden, chunks, per_load, lags),
            name="mlp",
            out_shape=jax.ShapeDtypeStruct((rows, cols), BF16),
            in_specs=[vmem] + [anywhere] * 6,
            out_specs=vmem,
            scratch_shapes=[
                VMEM((rows, cols), BF16), VMEM((cols,), BF16),
                VMEM((8, local_rows, q_cols), BF16), VMEM(w_o.shape, BF16),
                VMEM((ring, cols, per_load * 2 * half), BF16), VMEM((ring, cols, per_load * 2 * half), BF16), VMEM((loads, per_load, 2, half, cols), BF16),
                VMEM((2, rows, cols), BF16), VMEM((2, rows, cols), BF16), VMEM((8, rows), F32), VMEM((8, 8, rows), F32),
                VMEM((rows, cols), BF16), VMEM((rows, cols), BF16), VMEM((rows, cols), F32),
            ] + [VMEM((chunks, 2, 2, 2, 2, 16, half // 2), BF16)] * 3 + [
                VMEM((chunks, 2, 2, 2, 16, half // 2), BF16), VMEM((chunks, 2, 2, 16, half // 2), BF16), VMEM((chunks, 2, 2, 2, 2, 16, half // 2), BF16),
                DMA((3,)), DMA((ring,)), DMA((ring,)), DMA((loads,)), DMA((13,)), DMA((13,)), DMA((3,)), DMA((3,)), DMA((8,)), DMA((8,)),
            ] + [DMA((chunks,))] * 12,
            compiler_params=pltpu.CompilerParams(collective_id=1, has_side_effects=True, vmem_limit_bytes=int(52.5 * 2 ** 20)),
            cost_estimate=pl.CostEstimate(flops=60_000_000_000, bytes_accessed=57_000_000, transcendentals=0),
        )(attn, hbm(x_in), hbm(gain_mlp), hbm(w_o), hbm(w_gate), hbm(w_up), hbm(w_down.reshape(loads, per_load, 2, half, cols)))
        return x_out, k_flat.reshape(k_cache.shape), v_flat.reshape(v_cache.shape)

    return jax.shard_map(local_layer, mesh=mesh, in_specs=in_specs, out_specs=out_specs, check_vma=False)
```

```python
import functools

import jax
import jax.numpy as jnp
from jax import lax
from jax.experimental import pallas as pl
from jax.experimental.pallas import tpu as pltpu
from jax.sharding import PartitionSpec as P

HEAD = 128
NORM_EPS = 1e-6
ROPE_THETA = 1000000.0
MESH = pl.DeviceIdType.MESH
F32 = jnp.float32
BF16 = jnp.bfloat16
VMEM = pltpu.VMEM
DMA = pltpu.SemaphoreType.DMA


def neighbours(mx):
    core = lax.rem(mx, 2)
    chip = mx // 2
    x_pos = lax.rem(chip, 2)
    y_pos = chip // 2
    others = (y_pos * 2 + (1 - x_pos), (1 - y_pos) * 2 + x_pos, (1 - y_pos) * 2 + (1 - x_pos))
    return core, chip, chip * 2 + (1 - core), others


def far_first(mx):
    core, chip, partner, others = neighbours(mx)
    return [other * 2 + c for other in (others[2], others[0], others[1]) for c in (core, 1 - core)] + [partner]


def hbm(array):
    return pltpu.with_memory_space_constraint(array, pltpu.HBM)


def send(src, dst, send_sem, recv_sem, my, mx):
    copy = pltpu.make_async_remote_copy(src_ref=src, dst_ref=dst, send_sem=send_sem, recv_sem=recv_sem, device_id=(my, mx), device_id_type=MESH)
    copy.start()
    return copy


def drain(ref, sem):
    pltpu.make_async_copy(ref, ref, sem).wait()


def share_stat(square_sum, my, mx, stat_out, stat_in, send_sems, recv_sems, between=None):
    rows = square_sum.shape[0]
    turned = jnp.transpose(jnp.broadcast_to(square_sum, (rows, 128)))[0:8]
    stat_out[...] = turned
    copies = []
    for step, peer in enumerate(far_first(mx)):
        copies.append(send(stat_out, stat_in.at[mx], send_sems.at[step], recv_sems.at[step], my, peer))
    stat_in[mx] = turned
    if between is not None:
        between()
    for copy in copies:
        copy.wait()
    total = jnp.sum(stat_in[...], axis=0)
    return jnp.transpose(jnp.broadcast_to(total[0:1], (128, rows)))[:, 0:1]


def enter(my, mx, with_z, meanwhile=None):
    barrier = pltpu.get_barrier_semaphore()
    for step in range(1, 8):
        pl.semaphore_signal(barrier, inc=1, device_id=(my, lax.rem(mx + step, 8)), device_id_type=MESH)
    if with_z:
        pl.semaphore_signal(barrier, inc=1, device_id=(1 - my, mx), device_id_type=MESH)
    if meanwhile is not None:
        meanwhile()
    pl.semaphore_wait(barrier, 8 if with_z else 7)


def qkv_kernel(hidden, pieces, freq_ref, lens_hbm, x_hbm, gain_hbm, wq_hbm, wk_hbm, wv_hbm, bq_hbm, bk_hbm, bv_hbm, out_ref,
               lens_s, x_v, gain_v, wq_v, wk_v, wv_v, bq_v, bk_v, bv_v, cos_v, sin_v, part, pair_in, chip_in, direct_in, stat_out, stat_in,
               w_sems, stat_send, stat_recv, pair_send, pair_recv, chip_send, chip_recv, direct_send, direct_recv):
    my = lax.axis_index("my")
    mx = lax.axis_index("mx")
    core, chip, partner, others = neighbours(mx)
    loads = [pltpu.make_async_copy(src, dst, w_sems.at[n]) for n, (src, dst) in enumerate((
        (wq_hbm, wq_v), (wk_hbm, wk_v), (wv_hbm, wv_v), (x_hbm, x_v), (gain_hbm, gain_v), (lens_hbm, lens_s), (bq_hbm, bq_v), (bk_hbm, bk_v), (bv_hbm, bv_v)))]
    loads[3].start()

    def meanwhile():
        for n in (4, 5, 0, 1, 2, 6, 7, 8):
            loads[n].start()
        loads[3].wait()

    enter(my, mx, False, meanwhile)
    x = x_v[...].astype(F32)
    square_sum = jnp.sum(x * x, axis=1, keepdims=True)

    def tables():
        loads[4].wait()
        loads[5].wait()
        rows = lens_s.shape[0]
        sub = lax.broadcasted_iota(jnp.int32, (rows, HEAD // 2), 0)
        position = jnp.zeros((rows, HEAD // 2), F32)
        for b in range(rows):
            position = jnp.where(sub == b, lens_s[b].astype(F32), position)
        angles = position * freq_ref[...][None, :]
        cos_half = jnp.cos(angles)
        sin_half = jnp.sin(angles)
        cos_v[...] = jnp.concatenate([cos_half, cos_half], axis=1)
        sin_v[...] = jnp.concatenate([-sin_half, sin_half], axis=1)
        for n in (0, 1, 2, 6, 7, 8):
            loads[n].wait()

    stat = share_stat(square_sum, my, mx, stat_out, stat_in, stat_send, stat_recv, tables)
    normed = (x * lax.rsqrt(stat / hidden + NORM_EPS) * gain_v[...].astype(F32)[None, :]).astype(BF16)
    weights = (wq_v, wk_v, wv_v)
    biases = (bq_v, bk_v, bv_v)
    copies = []
    pair_copies = []
    direct = []
    for n, (which, first, width, out_first) in enumerate(pieces):
        cols = pl.ds(out_first, width)
        product = jnp.dot(normed, weights[which][:, first:first + width], preferred_element_type=F32)
        part[:, :, :, cols] = product.reshape(4, 2, 8, width).astype(BF16)
        if n == 0:
            for k, peer in enumerate(far_first(mx)):
                direct.append(send(part.at[peer // 2, lax.rem(peer, 2), :, cols], direct_in.at[k], direct_send.at[k], direct_recv.at[k], my, peer))
        else:
            pair_copies.append(send(part.at[:, 1 - core, :, cols], pair_in.at[:, :, cols], pair_send.at[n - 1], pair_recv.at[n - 1], my, partner))
    for n, (which, first, width, out_first) in enumerate(pieces[1:]):
        cols = pl.ds(out_first, width)
        pair_copies[n].wait_recv()
        pair_in[:, :, cols] = (part[:, core, :, cols].astype(F32) + pair_in[:, :, cols].astype(F32)).astype(BF16)
        for k, other in enumerate(others):
            copies.append(send(pair_in.at[other, :, cols], chip_in.at[k, :, cols], chip_send.at[n, k], chip_recv.at[n, k], my, other * 2 + core))
    for n, (which, first, width, out_first) in enumerate(pieces):
        cols = pl.ds(out_first, width)
        if n == 0:
            total = part[chip, core, :, cols].astype(F32)
            for k in range(7):
                direct[k].wait_recv()
                total = total + direct_in[k].astype(F32)
        else:
            total = pair_in[chip, :, cols].astype(F32)
            for k in range(3):
                copies[(n - 1) * 3 + k].wait_recv()
                total = total + chip_in[k, :, cols].astype(F32)
        total = total + biases[which][first:first + width].astype(F32)[None, :]
        for h in range(0, width, HEAD):
            vals = total[:, h:h + HEAD]
            if which < 2:
                vals = vals * cos_v[...] + pltpu.roll(vals, HEAD // 2, 1) * sin_v[...]
            out_ref[:, out_first + h:out_first + h + HEAD] = vals
    for copy in direct + pair_copies + copies:
        copy.wait_send()


def attend_kernel(heads, proj_ref, k_ref, v_ref, lens_hbm, ko_hbm, vo_hbm, attn_ref,
                  lens_s, q_s, k_s, v_s, o_s, k_win, v_win, lens_sem, out_sems, win_sems):
    rows, slots, _ = k_ref.shape
    q_cols = heads * HEAD
    kv_cols = (proj_ref.shape[1] - q_cols) // 2
    kv_heads = kv_cols // HEAD
    group = heads // kv_heads
    load_lens = pltpu.make_async_copy(lens_hbm, lens_s, lens_sem)
    load_lens.start()
    outs = []
    for b in range(rows):
        outs.append((pltpu.make_async_copy(k_ref.at[b], ko_hbm.at[b], out_sems.at[0, b]), pltpu.make_async_copy(v_ref.at[b], vo_hbm.at[b], out_sems.at[1, b])))
        for out in outs[b]:
            out.start()
    q_s[...] = jnp.zeros_like(q_s)
    for h in range(heads):
        q_s[:, h, :] = proj_ref[:, h * HEAD:(h + 1) * HEAD]
    for h in range(kv_heads):
        k_new = proj_ref[:, q_cols + h * HEAD:q_cols + (h + 1) * HEAD]
        v_new = proj_ref[:, q_cols + kv_cols + h * HEAD:q_cols + kv_cols + (h + 1) * HEAD]
        for r in range(16 // kv_heads):
            k_s[:, r * kv_heads + h, :] = k_new
            v_s[:, r * kv_heads + h, :] = v_new
    load_lens.wait()
    q_pad = q_s.shape[1]
    per_tile = 16 // kv_heads
    sub = lax.broadcasted_iota(jnp.int32, (16, HEAD), 0) // kv_heads
    row = lax.broadcasted_iota(jnp.int32, (q_pad, 1), 0)
    row_head = sum((row >= group * n).astype(jnp.int32) for n in range(1, kv_heads))
    col = lax.broadcasted_iota(jnp.int32, (q_pad, slots), 1)
    offset = jnp.where(lax.rem(col, kv_heads) == row_head, col // kv_heads, slots)
    new_col = lax.broadcasted_iota(jnp.int32, (q_pad, 16), 1)

    def window(b, position):
        base = pl.multiple_of(position // per_tile * 16, 16)
        at_slot = sub == lax.rem(position, per_tile)
        for src, new, win in ((k_ref, k_s, k_win), (v_ref, v_s, v_win)):
            win[b] = jnp.where(at_slot, new[b], src[b, pl.ds(base, 16), :].astype(F32)).astype(BF16)

    def one_row(b):
        position = lens_s[b]
        if b < rows - 1:
            window(b, position)
        query = q_s[b].astype(BF16)
        scores = lax.dot_general(query, k_ref[b], (((1,), (1,)), ((), ())), preferred_element_type=F32) * HEAD ** -0.5
        scores = jnp.where(offset < position, scores, -jnp.inf)
        new_scores = lax.dot_general(query, k_s[b].astype(BF16), (((1,), (1,)), ((), ())), preferred_element_type=F32) * HEAD ** -0.5
        new_scores = jnp.where(new_col == row_head, new_scores, -jnp.inf)
        top = jnp.maximum(jnp.max(scores, axis=1, keepdims=True), jnp.max(new_scores, axis=1, keepdims=True))
        weights = jnp.exp(scores - top)
        new_weights = jnp.exp(new_scores - top)
        weight_sum = jnp.sum(weights, axis=1, keepdims=True) + jnp.sum(new_weights, axis=1, keepdims=True)
        weighted = jnp.dot(weights.astype(BF16), v_ref[b], preferred_element_type=F32)
        weighted = weighted + jnp.dot(new_weights.astype(BF16), v_s[b].astype(BF16), preferred_element_type=F32)
        o_s[b] = weighted / weight_sum

    def fix(b):
        base = pl.multiple_of(lens_s[b] // per_tile * 16, 16)
        return [pltpu.make_async_copy(win.at[b], hbm_out.at[b, pl.ds(base, 16), :], win_sems.at[n, b]) for n, (win, hbm_out) in enumerate(((k_win, ko_hbm), (v_win, vo_hbm)))]

    for b in range(rows - 1):
        one_row(b)
    window(rows - 1, lens_s[rows - 1])
    for b in range(rows):
        for out, win in zip(outs[b], fix(b)):
            out.wait()
            win.start()
    one_row(rows - 1)
    for h in range(heads):
        attn_ref[:, h * HEAD:(h + 1) * HEAD] = o_s[:, h, :].astype(BF16)
    for b in range(rows):
        for win in fix(b):
            win.wait()


def mlp_kernel(hidden, chunks, per_load, lags, attn_ref, x_hbm, gain_hbm, wo_hbm, wg_hbm, wu_hbm, wd_hbm, out_ref,
               x_v, gain_v, attn_all, wo_v, wg_v, wu_v, wd_v, z_out, z_in, stat_out, stat_in, h_v, m_v, acc, mine, theirs, pair_in, hop_in, fin_in, act,
               in_sems, wg_sems, wu_sems, wd_sems, ag_send, ag_recv, z_send, z_recv, stat_send, stat_recv,
               pair_send, pair_recv, hop_send, hop_recv, fin_send, fin_recv, near_send, near_recv, far_send, far_recv, fwd_send, fwd_recv):
    my = lax.axis_index("my")
    mx = lax.axis_index("mx")
    core, chip, partner, others = neighbours(mx)
    x_pos = lax.rem(chip, 2)
    y_pos = chip // 2
    x_peer = others[0] * 2 + core
    y_peer = others[1] * 2 + core
    x_across = others[0] * 2 + (1 - core)
    y_across = others[1] * 2 + (1 - core)
    straight = chunks - 1
    half = 2 * act.shape[6]
    loads = chunks // per_load
    load_cols = per_load * 2 * half
    ring = wg_v.shape[0]

    def load_gate(n):
        cols = pl.ds(pl.multiple_of(n * load_cols, 128), load_cols)
        slot = lax.rem(n, ring)
        return pltpu.make_async_copy(wg_hbm.at[:, cols], wg_v.at[slot], wg_sems.at[slot]), pltpu.make_async_copy(wu_hbm.at[:, cols], wu_v.at[slot], wu_sems.at[slot])

    def load_down(n):
        return pltpu.make_async_copy(wd_hbm.at[n], wd_v.at[n], wd_sems.at[n])

    firsts = [pltpu.make_async_copy(src, dst, in_sems.at[n]) for n, (src, dst) in enumerate(((wo_hbm, wo_v), (x_hbm, x_v), (gain_hbm, gain_v)))]

    def meanwhile():
        for first in firsts:
            first.start()

        @pl.loop(0, ring)
        def _(n):
            for load in load_gate(n):
                load.start()

        @pl.loop(0, loads)
        def _(n):
            load_down(n).start()

        attn_all[mx] = attn_ref[...]
        acc[...] = jnp.zeros_like(acc)

    enter(my, mx, True, meanwhile)

    others = (others[2], others[0], others[1])
    shared = pl.ds(0, 12 * HEAD)
    direct = pl.ds(12 * HEAD, attn_ref.shape[1] - 12 * HEAD)
    spread = [send(attn_ref.at[:, shared], attn_all.at[mx, :, shared], ag_send.at[k], ag_recv.at[k], my, other * 2 + core) for k, other in enumerate(others)]
    passed = [send(attn_ref, attn_all.at[mx], ag_send.at[3], ag_recv.at[3], my, partner)]
    for k, other in enumerate(others):
        for n, peer in enumerate((other * 2 + core, other * 2 + (1 - core))):
            slot = 4 + 2 * k + n
            passed.append(send(attn_ref.at[:, direct], attn_all.at[mx, :, direct], ag_send.at[slot], ag_recv.at[slot], my, peer))
    for k, other in enumerate(others):
        spread[k].wait()
        block = attn_all.at[other * 2 + core, :, shared]
        passed.append(send(block, block, ag_send.at[10 + k], ag_recv.at[10 + k], my, partner))
    for first in firsts:
        first.wait()
    for copy in passed:
        copy.wait()
    rows = x_v.shape[0]
    attn = attn_all[...].reshape(rows, attn_ref.shape[1])
    z_parts = (pl.ds(0, 384), pl.ds(384, x_v.shape[1] - 384))
    z_copies = []
    for n, part in enumerate(z_parts):
        z_out[0, :, part] = jnp.dot(attn, wo_v[:, part], preferred_element_type=F32).astype(BF16)
        z_copies.append(send(z_out.at[0, :, part], z_in.at[0, :, part], z_send.at[n], z_recv.at[n], 1 - my, mx))
    for z_copy in z_copies:
        z_copy.wait()
    mid = (x_v[...].astype(F32) + (z_out[0].astype(F32) + z_in[0].astype(F32))).astype(BF16)
    m_v[...] = mid
    mid = mid.astype(F32)
    stat = share_stat(jnp.sum(mid * mid, axis=1, keepdims=True), my, mx, stat_out, stat_in, stat_send, stat_recv)
    h_v[...] = (mid * lax.rsqrt(stat / hidden + NORM_EPS) * gain_v[...].astype(F32)[None, :]).astype(BF16)

    def multiply(k):
        n = k // per_load
        slot = lax.rem(n, ring)
        step = lax.rem(k, per_load)

        @pl.when(step == 0)
        def _():
            for load in load_gate(n):
                load.wait()

        h = h_v[...]

        def products(part, dest):
            cols = pl.ds(pl.multiple_of(step * (2 * half) + part * half, 128), half)
            for which, weights in ((0, wg_v), (1, wu_v)):
                out = jnp.dot(h, weights[slot, :, cols], preferred_element_type=F32).astype(BF16)
                for way in range(2):
                    dest[k, way, :, :, which] = out[:, way * half // 2:(way + 1) * half // 2].reshape(2, 2, 16, half // 2)

        products(1 - core, theirs)
        send(theirs.at[k], pair_in.at[k], pair_send.at[k], pair_recv.at[k], my, partner)
        products(core, mine)

        @pl.when(jnp.logical_and(step == per_load - 1, n + ring < loads))
        def _():
            for load in load_gate(n + ring):
                load.start()

    def scatter(k):
        drain(pair_in.at[k], pair_recv.at[k])
        pair_in[k] = (mine[k].astype(F32) + pair_in[k].astype(F32)).astype(BF16)
        send(pair_in.at[k, 0, :, 1 - x_pos], hop_in.at[k, 0], hop_send.at[k], hop_recv.at[k], my, x_peer)
        send(pair_in.at[k, 1, 1 - y_pos], hop_in.at[k, 1], hop_send.at[k], hop_recv.at[k], my, y_peer)

    def combine(k):
        drain(hop_in.at[k], hop_recv.at[k])
        hop_in[k, 0] = (pair_in[k, 0, :, x_pos].astype(F32) + hop_in[k, 0].astype(F32)).astype(BF16)
        hop_in[k, 1] = (pair_in[k, 1, y_pos].astype(F32) + hop_in[k, 1].astype(F32)).astype(BF16)
        send(hop_in.at[k, 0, 1 - y_pos], fin_in.at[k, 0], fin_send.at[k], fin_recv.at[k], my, y_peer)
        send(hop_in.at[k, 1, 1 - x_pos], fin_in.at[k, 1], fin_send.at[k], fin_recv.at[k], my, x_peer)

    def activate(k):
        drain(fin_in.at[k], fin_recv.at[k])
        for way, own in ((0, y_pos), (1, x_pos)):
            total = hop_in[k, way, own].astype(F32) + fin_in[k, way].astype(F32)
            gate = total[0]
            act[k, core, way, y_pos, x_pos] = (gate * jax.nn.sigmoid(gate) * total[1]).astype(BF16)
        for way, peer in ((0, y_peer), (1, x_peer)):
            block = act.at[k, core, way, y_pos, x_pos]
            send(block, block, near_send.at[k], near_recv.at[k], my, peer)
        both = act.at[k, core, :, y_pos, x_pos]
        send(both, both, fwd_send.at[k], fwd_recv.at[k], my, partner)

    def gather(k):
        drain(act.at[k, core, 0, 0], near_recv.at[k])
        for block, peer in ((act.at[k, core, 0, :, x_pos], x_peer), (act.at[k, core, 1, y_pos], y_peer)):
            send(block, block, far_send.at[k], far_recv.at[k], my, peer)
        for block in (act.at[k, core, 0, 1 - y_pos, x_pos], act.at[k, core, 1, y_pos, 1 - x_pos]):
            send(block, block, fwd_send.at[k], fwd_recv.at[k], my, partner)

        @pl.when(k >= straight)
        def _():
            for block, peer in ((act.at[k, core, 0, :, x_pos], x_across), (act.at[k, core, 1, y_pos], y_across)):
                send(block, block, fwd_send.at[k], fwd_recv.at[k], my, peer)

    def forward(k):
        drain(act.at[k, core, 0], far_recv.at[k])

        @pl.when(k < straight)
        def _():
            for block in (act.at[k, core, 0, :, 1 - x_pos], act.at[k, core, 1, 1 - y_pos]):
                send(block, block, fwd_send.at[k], fwd_recv.at[k], my, partner)

    def contract(k):
        n = k // per_load
        step = lax.rem(k, per_load)

        @pl.when(step == 0)
        def _():
            load_down(n).wait()

        drain(act.at[k, 1 - core], fwd_recv.at[k])
        total = acc[...]
        for part in range(2):
            lhs = jnp.concatenate([act[k, part, way].reshape(rows, half // 2) for way in range(2)], axis=1)
            total = total + jnp.dot(lhs, wd_v[n, step, part], preferred_element_type=F32)
        acc[...] = total

    stages = tuple(zip((forward, gather, activate, combine, scatter, contract, multiply), lags))

    @pl.loop(0, chunks + max(lags))
    def _(t):
        for stage, lag in stages:
            @pl.when(jnp.logical_and(t >= lag, t < chunks + lag))
            def _():
                stage(t - lag)

    z_out[1] = acc[...].astype(BF16)
    z_copy = send(z_out.at[1], z_in.at[1], z_send.at[2], z_recv.at[2], 1 - my, mx)
    z_copy.wait()
    out_ref[...] = (m_v[...].astype(F32) + (z_out[1].astype(F32) + z_in[1].astype(F32))).astype(BF16)

    @pl.loop(0, chunks)
    def _(k):
        drain(theirs.at[k], pair_send.at[k])
        drain(hop_in.at[k], hop_send.at[k])
        drain(fin_in.at[k], fin_send.at[k])
        drain(act.at[k, core, 0, 0], near_send.at[k])
        drain(act.at[k, core, 0], far_send.at[k])
        drain(act.at[k, core], fwd_send.at[k])


def solution(mesh):
    mx_size = mesh.shape["mx"]
    act_spec = P(None, "mx")
    cache_spec = P("mx", None, "my", None)
    in_specs = (act_spec, P("mx"), P("mx"), P("mx"), P("mx", "my"), P("my"), P("mx", "my"), P("my"), P("mx", "my"), P("my"), P("my", "mx"), P("mx", "my"), P("mx", "my"), P("my", "mx"), cache_spec, cache_spec)
    out_specs = (act_spec, cache_spec, cache_spec)
    vmem = pl.BlockSpec(memory_space=pltpu.VMEM)
    anywhere = pl.BlockSpec(memory_space=pl.ANY)

    def local_layer(x_in, seq_lens, gain_attn, gain_mlp, w_q, b_q, w_k, b_k, w_v, b_v, w_o, w_gate, w_up, w_down, k_cache, v_cache):
        rows, cols = x_in.shape
        hidden = cols * mx_size
        q_cols = w_q.shape[1]
        kv_cols = w_k.shape[1]
        heads = q_cols // HEAD
        kv_heads = kv_cols // HEAD
        local_rows = rows // mx_size
        qkv_cols = q_cols + 2 * kv_cols
        first = 8 * HEAD
        rest = (q_cols - first) // 2
        pieces = ((0, 0, first, 0), (0, first, rest, first), (0, first + rest, rest, first + rest), (1, 0, kv_cols, q_cols), (2, 0, kv_cols, q_cols + kv_cols))
        inv_freq = ROPE_THETA ** (-2.0 * jnp.arange(HEAD // 2, dtype=F32) / HEAD)

        projected = pl.pallas_call(
            functools.partial(qkv_kernel, hidden, pieces),
            name="qkv",
            out_shape=jax.ShapeDtypeStruct((local_rows, qkv_cols), F32),
            in_specs=[vmem] + [anywhere] * 9,
            out_specs=vmem,
            scratch_shapes=[
                pltpu.SMEM((local_rows,), jnp.int32), VMEM((rows, cols), BF16), VMEM((cols,), BF16),
                VMEM(w_q.shape, BF16), VMEM(w_k.shape, BF16), VMEM(w_v.shape, BF16), VMEM(b_q.shape, BF16), VMEM(b_k.shape, BF16), VMEM(b_v.shape, BF16),
                VMEM((local_rows, HEAD), F32), VMEM((local_rows, HEAD), F32),
                VMEM((4, 2, local_rows, qkv_cols), BF16), VMEM((4, local_rows, qkv_cols), BF16), VMEM((3, local_rows, qkv_cols), BF16), VMEM((7, local_rows, first), BF16),
                VMEM((8, rows), F32), VMEM((8, 8, rows), F32),
                DMA((9,)), DMA((8,)), DMA((8,)), DMA((4,)), DMA((4,)), DMA((4, 3)), DMA((4, 3)), DMA((7,)), DMA((7,)),
            ],
            compiler_params=pltpu.CompilerParams(collective_id=0, has_side_effects=True, vmem_limit_bytes=16 * 2 ** 20),
            cost_estimate=pl.CostEstimate(flops=40_000_000_000, bytes_accessed=4_600_000, transcendentals=0),
        )(inv_freq, hbm(seq_lens), hbm(x_in), hbm(gain_attn), hbm(w_q), hbm(w_k), hbm(w_v), hbm(b_q), hbm(b_k), hbm(b_v))

        slots = k_cache.shape[1] * kv_heads
        flat = (local_rows, slots, HEAD)
        padded = (heads + 7) // 8 * 8
        k_flat, v_flat, attn = pl.pallas_call(
            functools.partial(attend_kernel, heads),
            name="attend",
            out_shape=(jax.ShapeDtypeStruct(flat, BF16), jax.ShapeDtypeStruct(flat, BF16), jax.ShapeDtypeStruct((local_rows, q_cols), BF16)),
            in_specs=[vmem] * 3 + [anywhere],
            out_specs=(anywhere, anywhere, vmem),
            scratch_shapes=[
                pltpu.SMEM((local_rows,), jnp.int32),
                VMEM((local_rows, padded, HEAD), F32), VMEM((local_rows, 16, HEAD), F32), VMEM((local_rows, 16, HEAD), F32), VMEM((local_rows, padded, HEAD), F32),
                VMEM((local_rows, 16, HEAD), BF16), VMEM((local_rows, 16, HEAD), BF16),
                DMA, DMA((2, local_rows)), DMA((2, local_rows)),
            ],
            compiler_params=pltpu.CompilerParams(vmem_limit_bytes=26 * 2 ** 20),
            cost_estimate=pl.CostEstimate(flops=20_000_000_000, bytes_accessed=17_000_000, transcendentals=0),
        )(projected, pltpu.with_memory_space_constraint(k_cache.reshape(flat), VMEM), pltpu.with_memory_space_constraint(v_cache.reshape(flat), VMEM), hbm(seq_lens))

        ff_cols = w_gate.shape[1]
        half = 768
        chunks = ff_cols // (2 * half)
        per_load = 1
        ring = 6
        loads = chunks // per_load
        lags = (20, 15, 10, 6, 2, 23, 0)
        x_out = pl.pallas_call(
            functools.partial(mlp_kernel, hidden, chunks, per_load, lags),
            name="mlp",
            out_shape=jax.ShapeDtypeStruct((rows, cols), BF16),
            in_specs=[vmem] + [anywhere] * 6,
            out_specs=vmem,
            scratch_shapes=[
                VMEM((rows, cols), BF16), VMEM((cols,), BF16),
                VMEM((8, local_rows, q_cols), BF16), VMEM(w_o.shape, BF16),
                VMEM((ring, cols, per_load * 2 * half), BF16), VMEM((ring, cols, per_load * 2 * half), BF16), VMEM((loads, per_load, 2, half, cols), BF16),
                VMEM((2, rows, cols), BF16), VMEM((2, rows, cols), BF16), VMEM((8, rows), F32), VMEM((8, 8, rows), F32),
                VMEM((rows, cols), BF16), VMEM((rows, cols), BF16), VMEM((rows, cols), F32),
            ] + [VMEM((chunks, 2, 2, 2, 2, 16, half // 2), BF16)] * 3 + [
                VMEM((chunks, 2, 2, 2, 16, half // 2), BF16), VMEM((chunks, 2, 2, 16, half // 2), BF16), VMEM((chunks, 2, 2, 2, 2, 16, half // 2), BF16),
                DMA((3,)), DMA((ring,)), DMA((ring,)), DMA((loads,)), DMA((13,)), DMA((13,)), DMA((3,)), DMA((3,)), DMA((8,)), DMA((8,)),
            ] + [DMA((chunks,))] * 12,
            compiler_params=pltpu.CompilerParams(collective_id=1, has_side_effects=True, vmem_limit_bytes=int(52.5 * 2 ** 20)),
            cost_estimate=pl.CostEstimate(flops=60_000_000_000, bytes_accessed=57_000_000, transcendentals=0),
        )(attn, hbm(x_in), hbm(gain_mlp), hbm(w_o), hbm(w_gate), hbm(w_up), hbm(w_down.reshape(loads, per_load, 2, half, cols)))
        return x_out, k_flat.reshape(k_cache.shape), v_flat.reshape(v_cache.shape)

    return jax.shard_map(local_layer, mesh=mesh, in_specs=in_specs, out_specs=out_specs, check_vma=False)
```
